8 devices in a mesh: data: 1 (over z), model: 2 (over y), seq: 4 (over x, core).
Axes of the slice: x: 2, y: 2, z: 1, core: 2. Of those that a mesh axis runs over, the one named last changes fastest.
Arguments:
- tokens: bfloat16 [64, 4096, 384], P('data', 'seq')
- lengths: int32 [64], P('data')
- slot_params: bfloat16 [384, 256], replicated
- logit_scale: float32 [], replicated
- w_in: bfloat16 [256, 384, 1536], P('seq', None, 'model')
- w_out: bfloat16 [256, 1536, 384], P('seq', 'model')
Outputs:
- output: bfloat16 [64, 4096, 384], P('data', 'seq')
All inputs are finite; a program needn't handle non-finite values.
Results may differ from the reference program's by a relative error of at most 0.0158228.
Values are sent between devices in bfloat16 or wider.
A program may use at most 1 GiB of HBM per device.

```python
import math
import jax
import jax.numpy as jnp
from jax import lax

BATCH_SIZE = 64
SEQ_LEN = 4096
MODEL_DIM = 384
HIDDEN_DIM = 1536
NUM_EXPERTS = 256
EXPERT_SLOTS = 1
NUM_SLOTS_TOTAL = NUM_EXPERTS * EXPERT_SLOTS
NORM_EPS = 1e-6


def setup_inputs(seed: int = 0, part: int = 0) -> dict:
    root_key = jax.random.key(seed)
    key_phi, key_gain, key_win, key_wout, key_part = jax.random.split(root_key, 5)
    part_key = jax.random.fold_in(key_part, part)
    key_tok, key_len = jax.random.split(part_key, 2)
    tokens = jax.random.normal(key_tok, (BATCH_SIZE, SEQ_LEN, MODEL_DIM), jnp.float32).astype(jnp.bfloat16)
    drawn = jax.random.randint(key_len, (BATCH_SIZE,), SEQ_LEN // 4, SEQ_LEN + 1, jnp.int32)
    lengths = jnp.where(jnp.arange(BATCH_SIZE) == 0, SEQ_LEN, drawn).astype(jnp.int32)
    slot_params = jax.random.normal(key_phi, (MODEL_DIM, NUM_SLOTS_TOTAL), jnp.float32).astype(jnp.bfloat16)
    logit_scale = math.sqrt(MODEL_DIM) * jax.random.uniform(key_gain, (), jnp.float32, 1.0, 2.0)
    in_scale = math.sqrt(SEQ_LEN) / (4.0 * math.sqrt(MODEL_DIM))
    w_in = (jax.random.normal(key_win, (NUM_EXPERTS, MODEL_DIM, HIDDEN_DIM), jnp.float32) * in_scale).astype(jnp.bfloat16)
    w_out = (jax.random.normal(key_wout, (NUM_EXPERTS, HIDDEN_DIM, MODEL_DIM), jnp.float32) / math.sqrt(HIDDEN_DIM)).astype(jnp.bfloat16)
    return {"tokens": tokens, "lengths": lengths, "slot_params": slot_params, "logit_scale": logit_scale, "w_in": w_in, "w_out": w_out}


def unit_vectors(values, axis):
    v32 = values.astype(jnp.float32)
    return (v32 * lax.rsqrt(jnp.sum(v32 * v32, axis=axis, keepdims=True) + NORM_EPS)).astype(jnp.bfloat16)


def reference(tokens, lengths, slot_params, logit_scale, w_in, w_out):
    slot_unit = unit_vectors(slot_params, 0)
    positions = jnp.arange(SEQ_LEN)

    def seq_logits(seq_tokens):
        return logit_scale * jnp.dot(unit_vectors(seq_tokens, 1), slot_unit, preferred_element_type=jnp.float32)

    def dispatch(args):
        seq_tokens, seq_length = args
        logits = seq_logits(seq_tokens)
        masked = jnp.where((positions < seq_length)[:, None], logits, -1e30)
        weights = jnp.exp(masked - jnp.max(masked, axis=0, keepdims=True))
        col_sum = jnp.sum(weights, axis=0)
        slot_sum = jnp.dot(weights.astype(jnp.bfloat16).T, seq_tokens, preferred_element_type=jnp.float32)
        return (slot_sum / col_sum[:, None]).astype(jnp.bfloat16)

    slot_in = lax.map(dispatch, (tokens, lengths))
    per_expert = slot_in.reshape(BATCH_SIZE, NUM_EXPERTS, EXPERT_SLOTS, MODEL_DIM).transpose(1, 0, 2, 3).reshape(NUM_EXPERTS, BATCH_SIZE * EXPERT_SLOTS, MODEL_DIM)

    def expert_ffn(args):
        rows, first, second = args
        hidden = jax.nn.gelu(jnp.dot(rows, first, preferred_element_type=jnp.float32), approximate=False).astype(jnp.bfloat16)
        return jnp.dot(hidden, second, preferred_element_type=jnp.float32).astype(jnp.bfloat16)

    expert_out = lax.map(expert_ffn, (per_expert, w_in, w_out))
    slot_out = expert_out.reshape(NUM_EXPERTS, BATCH_SIZE, EXPERT_SLOTS, MODEL_DIM).transpose(1, 0, 2, 3).reshape(BATCH_SIZE, NUM_SLOTS_TOTAL, MODEL_DIM)

    def combine(args):
        seq_tokens, seq_length, seq_slots = args
        mix_weights = jax.nn.softmax(seq_logits(seq_tokens), axis=1).astype(jnp.bfloat16)
        mixed = jnp.dot(mix_weights, seq_slots, preferred_element_type=jnp.float32)
        return jnp.where((positions < seq_length)[:, None], mixed, 0.0).astype(jnp.bfloat16)

    return lax.map(combine, (tokens, lengths, slot_out))
```

```python
import functools
import math
import jax
import jax.numpy as jnp
from jax import lax
from jax.experimental import pallas as pl
from jax.experimental.pallas import tpu as pltpu
from jax.sharding import PartitionSpec as P

NORM_EPS = 1e-6
LOG2E = math.log2(math.e)
MASKED = -1e30
MESH = pl.DeviceIdType.MESH
F32, BF16 = jnp.float32, jnp.bfloat16
NT = (((1,), (1,)), ((), ()))


def unit_vectors(values, axis):
    v32 = values.astype(F32)
    return (v32 * lax.rsqrt(jnp.sum(v32 * v32, axis=axis, keepdims=True) + NORM_EPS)).astype(BF16)


def place():
    y, s = lax.axis_index("model"), lax.axis_index("seq")
    x, core = s // 2, lax.rem(s, 2)
    partner = (0, y, x * 2 + 1 - core)
    across_x = (0, y, (1 - x) * 2 + core)
    across_y = (0, 1 - y, s)
    return y, x, core, s, partner, across_x, across_y


def greet(devices):
    barrier = pltpu.get_barrier_semaphore()
    for device in devices:
        pl.semaphore_signal(barrier, inc=1, device_id=device, device_id_type=MESH)
    pl.semaphore_wait(barrier, len(devices))


def remote(src, dst, send, recv, device):
    return pltpu.make_async_remote_copy(src_ref=src, dst_ref=dst, send_sem=send, recv_sem=recv, device_id=device, device_id_type=MESH)


def merge_weights(a, b):
    top = jnp.maximum(a, b)
    ea, eb = jnp.exp2(a - top), jnp.exp2(b - top)
    total = ea + eb
    row = lax.broadcasted_iota(jnp.int32, (8, a.shape[1]), 0)
    weights = jnp.where(row == 0, ea / total, eb / total)
    return jnp.transpose(weights), top + jnp.log2(total)


def scatter_rows(acc, first, stride, rows):
    for j in range(acc.shape[0]):
        acc[j, pl.ds(first, rows.shape[0], stride=stride), :] = rows[:, j * 128 : (j + 1) * 128]


def gather_rows(acc, rows):
    return jnp.concatenate([acc[j, rows, :] for j in range(acc.shape[0])], axis=1)


def dispatch_kernel(half, x_hbm, vt_ref, len_ref, kg_ref, xs_ref, xbuf, part, dpart, mid, xpart, own, yown, acc, lse, dlse, mlse, xlse, wcol, in_sem, d_s, d_r, dl_s, dl_r, x_s, x_r, xl_s, xl_r, y_s, y_r):
    tok, n_slots, dim = xbuf.shape[1], vt_ref.shape[0], xbuf.shape[2]
    core_slots, dev_slots = n_slots // 2, n_slots // 4
    n_batch = 2 * half
    y, x, core, s, partner, across_x, across_y = place()
    base = y * half
    ring = xbuf.shape[0]

    def load(i):
        slot = lax.rem(i, ring)
        return pltpu.make_async_copy(x_hbm.at[base + i], xbuf.at[slot], in_sem.at[slot])

    def core_copy(i):
        rows = pl.ds(pl.multiple_of((1 - core) * core_slots, core_slots), core_slots)
        return remote(part.at[i, rows], dpart.at[i], d_s.at[i], d_r.at[i], partner)

    def core_lse(i):
        return remote(lse.at[i, 1 - core], dlse.at[i], dl_s.at[i], dl_r.at[i], partner)

    def x_copy(i):
        rows = pl.ds(pl.multiple_of((1 - x) * dev_slots, dev_slots), dev_slots)
        return remote(mid.at[i, rows], xpart.at[i], x_s.at[i], x_r.at[i], across_x)

    def x_lse(i):
        return remote(mlse.at[i], xlse.at[i], xl_s.at[i], xl_r.at[i], across_x)

    def y_copy(i):
        return remote(own.at[i], yown.at[i], y_s.at[i], y_r.at[i], across_y)

    for i in range(ring):
        load(i).start()
    greet((partner, across_x, across_y))

    def step(i, carry):
        @pl.when(i < half)
        def _():
            load(i).wait()
            slot = lax.rem(i, ring)
            xv = xbuf[slot]
            xf = xv.astype(F32)
            square = jnp.sum(xf * xf, axis=1, keepdims=True)
            square_row = jnp.transpose(jnp.broadcast_to(square, (tok, 128)))[0:1]
            scale_row = lax.rsqrt(square_row + NORM_EPS) * kg_ref[0]
            logits = lax.dot_general(vt_ref[...], xv, NT, preferred_element_type=F32) * scale_row
            lane = lax.broadcasted_iota(jnp.int32, (1, tok), 1)
            masked = jnp.where(lane < len_ref[base + i] - s * tok, logits, MASKED)
            top = jnp.max(masked, axis=1, keepdims=True)
            weights = jnp.exp2(masked - top)
            total = jnp.sum(weights, axis=1, keepdims=True)
            mean = jnp.dot(weights.astype(BF16), xv, preferred_element_type=F32) * (1.0 / total)
            part[i] = mean.astype(BF16)
            first = lax.broadcasted_iota(jnp.int32, (n_slots, 128), 1) == 0
            rows = jnp.transpose(jnp.where(first, top, total))
            row = rows[0:1] + jnp.log2(rows[1:2])
            lse[i, 0] = row[:, :128]
            lse[i, 1] = row[:, 128:]
            core_copy(i).start()
            core_lse(i).start()

            @pl.when(i + ring < half)
            def _():
                load(i + ring).start()

        @pl.when((i >= 1) & (i < half + 1))
        def _():
            k = i - 1
            core_copy(k).wait_recv()
            core_lse(k).wait_recv()
            cols, row = merge_weights(lse[k, core], dlse[k])
            rows = pl.ds(pl.multiple_of(core * core_slots, core_slots), core_slots)
            merged = cols[:, 0:1] * part[k, rows].astype(F32) + cols[:, 1:2] * dpart[k].astype(F32)
            mid[k] = merged.astype(BF16)
            mlse[k] = row
            x_copy(k).start()
            x_lse(k).start()

        @pl.when((i >= 4) & (i < half + 4))
        def _():
            k = i - 4
            x_copy(k).wait_recv()
            x_lse(k).wait_recv()
            cols, _ = merge_weights(mlse[k], xlse[k])
            wcol[...] = cols
            rows = pl.ds(pl.multiple_of(x * dev_slots, dev_slots), dev_slots)
            mine = wcol[rows, :]
            merged = mine[:, 0:1] * mid[k, rows].astype(F32) + mine[:, 1:2] * xpart[k].astype(F32)
            own[k] = merged.astype(BF16)
            y_copy(k).start()
            scatter_rows(acc, base + k, n_batch, merged)

        @pl.when(i >= 7)
        def _():
            k = i - 7
            y_copy(k).wait_recv()
            scatter_rows(acc, (1 - y) * half + k, n_batch, yown[k].astype(F32))

        return carry

    lax.fori_loop(0, half + 7, step, 0)

    def flush(e, carry):
        rows = pl.ds(pl.multiple_of(e * n_batch, n_batch), n_batch)
        xs_ref[rows, :] = gather_rows(acc, rows).astype(BF16)
        return carry

    lax.fori_loop(0, dev_slots, flush, 0)

    def drain(i, carry):
        core_copy(i).wait_send()
        core_lse(i).wait_send()
        x_copy(i).wait_send()
        x_lse(i).wait_send()
        y_copy(i).wait_send()
        return carry

    lax.fori_loop(0, half, drain, 0)


def dispatch(tokens, vt, lengths, kg):
    n_batch, tok, dim = tokens.shape
    n_slots = vt.shape[0]
    half, ring = n_batch // 2, 4
    dma = pltpu.SemaphoreType.DMA
    return pl.pallas_call(
        functools.partial(dispatch_kernel, half),
        out_shape=pltpu.VMEM((n_slots // 4 * n_batch, dim), BF16),
        in_specs=[pl.BlockSpec(memory_space=pl.ANY), pl.BlockSpec(memory_space=pltpu.VMEM), pl.BlockSpec(memory_space=pltpu.SMEM), pl.BlockSpec(memory_space=pltpu.SMEM)],
        out_specs=pl.BlockSpec(memory_space=pltpu.VMEM),
        scratch_shapes=[
            pltpu.VMEM((ring, tok, dim), BF16),
            pltpu.VMEM((half, n_slots, dim), BF16),
            pltpu.VMEM((half, n_slots // 2, dim), BF16),
            pltpu.VMEM((half, n_slots // 2, dim), BF16),
            pltpu.VMEM((half, n_slots // 4, dim), BF16),
            pltpu.VMEM((half, n_slots // 4, dim), BF16),
            pltpu.VMEM((half, n_slots // 4, dim), BF16),
            pltpu.VMEM((dim // 128, n_slots // 4 * n_batch, 128), F32),
            pltpu.VMEM((half, 2, 1, n_slots // 2), F32),
            pltpu.VMEM((half, 1, n_slots // 2), F32),
            pltpu.VMEM((half, 1, n_slots // 2), F32),
            pltpu.VMEM((half, 1, n_slots // 2), F32),
            pltpu.VMEM((n_slots // 2, 8), F32),
            dma((ring,)),
        ] + [dma((half,))] * 10,
        compiler_params=pltpu.CompilerParams(collective_id=0, has_side_effects=True, vmem_limit_bytes=48 << 20),
        name="dispatch",
    )(tokens, vt, lengths, kg)


def expert_kernel(n_group, n_chunk, x_hbm, v_ref, len_ref, kg_ref, xs_ref, win_hbm, wout_hbm, c_ref, ys_hbm, xbuf, wi, wo, acc, ysend, yrecv, x_sem, wi_sem, wo_sem, y_s, y_r, x_s, x_r, d_s, d_r, r_s, r_r, l_s):
    n_batch, tok, dim = x_hbm.shape
    n_expert = win_hbm.shape[0]
    group = n_expert // n_group
    sub = n_batch // n_chunk
    core_slots, dev_slots = 2 * n_expert, n_expert
    y, x, core, s, partner, across_x, across_y = place()
    x_ring, w_ring = xbuf.shape[0], wi.shape[0]
    n_pair = n_expert // 2
    n_q = n_group * n_chunk

    def load_x(b):
        slot = lax.rem(b, x_ring)
        return pltpu.make_async_copy(x_hbm.at[b], xbuf.at[slot], x_sem.at[slot])

    def load_w(p):
        slot = lax.rem(p, w_ring)
        return (
            pltpu.make_async_copy(win_hbm.at[pl.ds(2 * p, 2)], wi.at[slot], wi_sem.at[slot]),
            pltpu.make_async_copy(wout_hbm.at[pl.ds(2 * p, 2)], wo.at[slot], wo_sem.at[slot]),
        )

    def home(q, on_core, on_x):
        g, bq = q // n_chunk, lax.rem(q, n_chunk)
        slot0 = pl.multiple_of(on_core * core_slots + on_x * dev_slots + g * group, group)
        return ys_hbm.at[pl.ds(bq * sub, sub), pl.ds(slot0, group)]

    def y_copy(q):
        return remote(ysend.at[q], yrecv.at[q], y_s.at[q], y_r.at[q], across_y)

    def x_copy(q):
        return remote(yrecv.at[q], home(q, core, x), x_s.at[q], x_r.at[q], across_x)

    def x_arrival(q):
        return remote(yrecv.at[q], home(q, core, 1 - x), x_s.at[q], x_r.at[q], across_x)

    def core_copy(q):
        return remote(yrecv.at[q], home(q, core, x), d_s.at[q], d_r.at[q], partner)

    def core_arrival(q):
        return remote(yrecv.at[q], home(q, 1 - core, x), d_s.at[q], d_r.at[q], partner)

    def relay(q):
        return remote(home(q, core, 1 - x), home(q, core, 1 - x), r_s.at[q], r_r.at[q], partner)

    def relay_arrival(q):
        return remote(home(q, 1 - core, 1 - x), home(q, 1 - core, 1 - x), r_s.at[q], r_r.at[q], partner)

    def local_copy(q):
        return pltpu.make_async_copy(yrecv.at[q], home(q, core, x), l_s.at[q])

    for p in range(w_ring):
        for copy in load_w(p):
            copy.start()
    for b in range(x_ring):
        load_x(b).start()
    greet((partner, across_x, across_y))

    def expert_pair(p, carry):
        for copy in load_w(p):
            copy.wait()
        slot = lax.rem(p, w_ring)
        for j in range(2):
            e = 2 * p + j
            rows = xs_ref[pl.ds(pl.multiple_of(e * n_batch, n_batch), n_batch), :]
            hidden = jnp.dot(rows, wi[slot, j], preferred_element_type=F32)
            hidden = (0.5 * hidden * (1.0 + lax.erf(hidden * math.sqrt(0.5)))).astype(BF16)
            out = jnp.dot(hidden, wo[slot, j], preferred_element_type=F32)
            scatter_rows(acc, lax.rem(e, group), group, out)

        @pl.when(p + w_ring < n_pair)
        def _():
            for copy in load_w(p + w_ring):
                copy.start()

        return carry

    def mix_block(b, carry):
        load_x(b).wait()
        slot = lax.rem(b, x_ring)
        xv = xbuf[slot]
        xf = xv.astype(F32)
        scale = lax.rsqrt(jnp.sum(xf * xf, axis=1, keepdims=True) + NORM_EPS) * kg_ref[0]
        logits = jnp.dot(xv, v_ref[...], preferred_element_type=F32) * scale
        weights = jnp.exp2(logits - jnp.max(logits, axis=1, keepdims=True))
        valid = lax.broadcasted_iota(jnp.int32, (tok, 1), 0) < len_ref[b] - s * tok
        inverse = jnp.where(valid, 1.0 / jnp.sum(weights, axis=1, keepdims=True), 0.0)
        c_ref[b] = (weights * inverse).astype(BF16)

        @pl.when(b + x_ring < n_batch)
        def _():
            load_x(b + x_ring).start()

        return carry

    per = n_expert // n_q

    def step(t, carry):
        @pl.when(t < n_q)
        def _():
            lax.fori_loop(t * (per // 2), (t + 1) * (per // 2), expert_pair, 0)

        @pl.when((t < n_q) & (lax.rem(t, n_chunk) == n_chunk - 1))
        def _():
            g = t // n_chunk

            def pack(bq, carry):
                rows = gather_rows(acc, pl.ds(pl.multiple_of(bq * sub * group, sub * group), sub * group))
                q = g * n_chunk + bq
                ysend[q] = rows.reshape(sub, group, dim).astype(BF16)
                y_copy(q).start()
                return carry

            lax.fori_loop(0, n_chunk, pack, 0)

        @pl.when((t >= n_chunk) & (t < n_q + n_chunk))
        def _():
            k = (t - n_chunk) * (n_batch // n_q)
            lax.fori_loop(k, k + n_batch // n_q, mix_block, 0)

        @pl.when((t >= n_chunk) & (t < n_q + n_chunk))
        def _():
            q = t - n_chunk
            y_copy(q).wait_recv()
            yrecv[q] = (ysend[q].astype(F32) + yrecv[q].astype(F32)).astype(BF16)
            x_copy(q).start()
            core_copy(q).start()
            local_copy(q).start()

        @pl.when(t >= n_chunk + 1)
        def _():
            q = t - n_chunk - 1
            x_arrival(q).wait_recv()
            relay(q).start()

        return carry

    lax.fori_loop(0, n_q + n_chunk + 1, step, 0)

    def drain(q, carry):
        core_arrival(q).wait_recv()
        relay_arrival(q).wait_recv()
        y_copy(q).wait_send()
        x_copy(q).wait_send()
        core_copy(q).wait_send()
        relay(q).wait_send()
        local_copy(q).wait()
        return carry

    lax.fori_loop(0, n_q, drain, 0)


def experts(tokens, v, lengths, kg, xs, w_in, w_out):
    n_batch, tok, dim = tokens.shape
    n_slots = v.shape[1]
    n_expert, _, hid = w_in.shape
    n_group, n_chunk = 4, 4
    group, sub = n_expert // n_group, n_batch // n_chunk
    n_q = n_group * n_chunk
    x_ring, w_ring = 3, 3
    dma = pltpu.SemaphoreType.DMA
    vmem, smem, anym = pl.BlockSpec(memory_space=pltpu.VMEM), pl.BlockSpec(memory_space=pltpu.SMEM), pl.BlockSpec(memory_space=pl.ANY)
    return pl.pallas_call(
        functools.partial(expert_kernel, n_group, n_chunk),
        out_shape=(pltpu.VMEM((n_batch, tok, n_slots), BF16), jax.ShapeDtypeStruct((n_batch, n_slots, dim), BF16)),
        in_specs=[anym, vmem, smem, smem, vmem, anym, anym],
        out_specs=(vmem, anym),
        scratch_shapes=[
            pltpu.VMEM((x_ring, tok, dim), BF16),
            pltpu.VMEM((w_ring, 2, dim, hid), BF16),
            pltpu.VMEM((w_ring, 2, hid, dim), BF16),
            pltpu.VMEM((dim // 128, group * n_batch, 128), F32),
            pltpu.VMEM((n_q, sub, group, dim), BF16),
            pltpu.VMEM((n_q, sub, group, dim), BF16),
            dma((x_ring,)),
            dma((w_ring,)),
            dma((w_ring,)),
        ] + [dma((n_q,))] * 9,
        compiler_params=pltpu.CompilerParams(collective_id=1, has_side_effects=True, vmem_limit_bytes=24 << 20),
        name="experts",
    )(tokens, v, lengths, kg, xs, w_in, w_out)


def combine_kernel(step, c_ref, ys_ref, y_ref):
    first = pl.program_id(0) * step
    for j in range(step):
        y_ref[j] = jnp.dot(c_ref[first + j], ys_ref[j], preferred_element_type=F32).astype(BF16)


def combine(c, ys):
    n_batch, tok, n_slots = c.shape
    dim = ys.shape[2]
    step = 4
    return pl.pallas_call(
        functools.partial(combine_kernel, step),
        grid=(n_batch // step,),
        out_shape=jax.ShapeDtypeStruct((n_batch, tok, dim), BF16),
        in_specs=[pl.BlockSpec(memory_space=pltpu.VMEM), pl.BlockSpec((step, n_slots, dim), lambda i: (i, 0, 0))],
        out_specs=pl.BlockSpec((step, tok, dim), lambda i: (i, 0, 0)),
        compiler_params=pltpu.CompilerParams(vmem_limit_bytes=24 << 20),
        name="combine",
    )(c, ys)


def solution(mesh):
    def local_layer(tokens, lengths, slot_params, logit_scale, w_in, w_out):
        dim, n_slots = slot_params.shape
        v = unit_vectors(slot_params, 0)
        v = v.reshape(dim, 2, 2, n_slots // 4).transpose(0, 2, 1, 3).reshape(dim, n_slots)
        kg = (logit_scale * LOG2E).reshape(1)
        xs = pltpu.with_memory_space_constraint(dispatch(tokens, v.T, lengths, kg), pltpu.VMEM)
        c, ys = experts(tokens, v, lengths, kg, xs, w_in, w_out)
        return combine(pltpu.with_memory_space_constraint(c, pltpu.VMEM), ys)

    return jax.shard_map(local_layer, mesh=mesh, in_specs=(P("data", "seq", None), P("data"), P(), P(), P("seq", None, "model"), P("seq", "model", None)), out_specs=P("data", "seq", None), check_vma=False)
```

```python
import functools
import math
import jax
import jax.numpy as jnp
from jax import lax
from jax.experimental import pallas as pl
from jax.experimental.pallas import tpu as pltpu
from jax.sharding import PartitionSpec as P

NORM_EPS = 1e-6
LOG2E = math.log2(math.e)
MASKED = -1e30
MESH = pl.DeviceIdType.MESH
F32, BF16 = jnp.float32, jnp.bfloat16
NT = (((1,), (1,)), ((), ()))


def unit_columns(values):
    v32 = values.astype(F32)
    return v32 * lax.rsqrt(jnp.sum(v32 * v32, axis=0, keepdims=True) + NORM_EPS)


def place():
    y, s = lax.axis_index("model"), lax.axis_index("seq")
    x, core = s // 2, lax.rem(s, 2)
    partner = (0, y, x * 2 + 1 - core)
    across_x = (0, y, (1 - x) * 2 + core)
    across_y = (0, 1 - y, s)
    return y, x, core, s, partner, across_x, across_y


def greet(devices):
    barrier = pltpu.get_barrier_semaphore()
    for device in devices:
        pl.semaphore_signal(barrier, inc=1, device_id=device, device_id_type=MESH)
    pl.semaphore_wait(barrier, len(devices))


def remote(src, dst, send, recv, device):
    return pltpu.make_async_remote_copy(src_ref=src, dst_ref=dst, send_sem=send, recv_sem=recv, device_id=device, device_id_type=MESH)


def merge_weights(a, b):
    top = jnp.maximum(a, b)
    ea, eb = jnp.exp2(a - top), jnp.exp2(b - top)
    total = ea + eb
    row = lax.broadcasted_iota(jnp.int32, (8, a.shape[1]), 0)
    weights = jnp.where(row == 0, ea, eb) * (1.0 / total)
    return jnp.transpose(weights), top + jnp.log2(total)


def scatter_rows(acc, first, stride, rows):
    for j in range(acc.shape[0]):
        acc[j, pl.ds(first, rows.shape[0], stride=stride), :] = rows[:, j * 128 : (j + 1) * 128]


def gather_rows(acc, rows):
    return jnp.concatenate([acc[j, rows, :] for j in range(acc.shape[0])], axis=1)


def dispatch_kernel(half, pitch, x_hbm, phi_ref, len_ref, g_ref, xs_ref, vt_ref, xbuf, part, mid, xpart, own, yown, lse, dlse, mlse, xlse, wcol, in_sem, d_s, d_r, dl_s, dl_r, x_s, x_r, xl_s, xl_r, y_s, y_r):
    size = part.shape[0] // d_s.shape[0]
    n_step = half // size
    tok, n_slots, dim = xbuf.shape[1], vt_ref.shape[0], xbuf.shape[2]
    core_slots, dev_slots = n_slots // 2, n_slots // 4
    y, x, core, s, partner, across_x, across_y = place()
    base = y * half
    ring = xbuf.shape[0]
    kg = g_ref[0] * LOG2E

    def load(i):
        slot = lax.rem(i, ring)
        return pltpu.make_async_copy(x_hbm.at[base + i], xbuf.at[slot], in_sem.at[slot])

    def core_copy(u):
        rows, some = pl.ds(pl.multiple_of((1 - core) * core_slots, core_slots), core_slots), pl.ds(u * size, size)
        return remote(part.at[some, rows], mid.at[some], d_s.at[u], d_r.at[u], partner)

    def core_lse(u):
        some = pl.ds(u * size, size)
        return remote(lse.at[1 - core, some], dlse.at[some], dl_s.at[u], dl_r.at[u], partner)

    def x_copy(u):
        rows, some = pl.ds(pl.multiple_of((1 - x) * dev_slots, dev_slots), dev_slots), pl.ds(u * size, size)
        return remote(mid.at[some, rows], xpart.at[some], x_s.at[u], x_r.at[u], across_x)

    def x_lse(u):
        some = pl.ds(u * size, size)
        return remote(mlse.at[some], xlse.at[some], xl_s.at[u], xl_r.at[u], across_x)

    def y_copy(u):
        some = pl.ds(u * size, size)
        return remote(own.at[some], yown.at[some], y_s.at[u], y_r.at[u], across_y)

    for i in range(ring):
        load(i).start()
    v_rows = jnp.transpose(unit_columns(phi_ref[...]))
    for j, block in enumerate((0, 2, 1, 3)):
        vt_ref[j * dev_slots : (j + 1) * dev_slots] = v_rows[block * dev_slots : (block + 1) * dev_slots].astype(BF16)
    greet((partner, across_x, across_y))

    def local_mean(i):
        xv = xbuf[lax.rem(i, ring)]
        xf = xv.astype(F32)
        square = jnp.sum(xf * xf, axis=1, keepdims=True)
        square_row = jnp.transpose(jnp.broadcast_to(square, (tok, 128)))[0:1]
        scale_row = lax.rsqrt(square_row + NORM_EPS) * kg
        logits = lax.dot_general(vt_ref[...], xv, NT, preferred_element_type=F32) * scale_row
        lane = lax.broadcasted_iota(jnp.int32, (1, tok), 1)
        masked = jnp.where(lane < len_ref[base + i] - s * tok, logits, MASKED)
        top = jnp.max(masked, axis=1, keepdims=True)
        weights = jnp.exp2(masked - top)
        total = jnp.sum(weights, axis=1, keepdims=True)
        mean = jnp.dot(weights.astype(BF16), xv, preferred_element_type=F32) * (1.0 / total)
        part[i] = mean.astype(BF16)
        first = lax.broadcasted_iota(jnp.int32, (n_slots, 128), 1) == 0
        rows = jnp.transpose(jnp.where(first, top, total))
        row = rows[0:1] + jnp.log2(rows[1:2])
        lse[0, i] = row[:, :core_slots]
        lse[1, i] = row[:, core_slots:]

    def step(u, carry):
        @pl.when(u < n_step)
        def _():
            for j in range(size):
                load(u * size + j).wait()
            for j in range(size):
                local_mean(u * size + j)
            core_copy(u).start()
            core_lse(u).start()

            @pl.when(u * size + ring < half)
            def _():
                for j in range(size):
                    load(u * size + j + ring).start()

        @pl.when((u >= 1) & (u < n_step + 1))
        def _():
            core_copy(u - 1).wait_recv()
            core_lse(u - 1).wait_recv()
            rows = pl.ds(pl.multiple_of(core * core_slots, core_slots), core_slots)
            for j in range(size):
                k = (u - 1) * size + j
                cols, row = merge_weights(lse[core, k], dlse[k])
                merged = cols[:, 0:1] * part[k, rows].astype(F32) + cols[:, 1:2] * mid[k].astype(F32)
                mid[k] = merged.astype(BF16)
                mlse[k] = row
            x_copy(u - 1).start()
            x_lse(u - 1).start()

        @pl.when((u >= 3) & (u < n_step + 3))
        def _():
            x_copy(u - 3).wait_recv()
            x_lse(u - 3).wait_recv()
            rows = pl.ds(pl.multiple_of(x * dev_slots, dev_slots), dev_slots)
            for j in range(size):
                k = (u - 3) * size + j
                cols, _ = merge_weights(mlse[k], xlse[k])
                wcol[j] = cols
                mine = wcol[j, rows, :]
                merged = mine[:, 0:1] * mid[k, rows].astype(F32) + mine[:, 1:2] * xpart[k].astype(F32)
                own[k] = merged.astype(BF16)
                scatter_rows(xs_ref, base + k, pitch, merged)
            y_copy(u - 3).start()

        @pl.when(u >= 5)
        def _():
            y_copy(u - 5).wait_recv()
            for j in range(size):
                k = (u - 5) * size + j
                scatter_rows(xs_ref, (1 - y) * half + k, pitch, yown[k].astype(F32))

        return carry

    lax.fori_loop(0, n_step + 5, step, 0)

    def drain(u, carry):
        core_copy(u).wait_send()
        core_lse(u).wait_send()
        x_copy(u).wait_send()
        x_lse(u).wait_send()
        y_copy(u).wait_send()
        return carry

    lax.fori_loop(0, n_step, drain, 0)


def dispatch(tokens, phi, lengths, g, pitch):
    n_batch, tok, dim = tokens.shape
    n_slots = phi.shape[1]
    half, ring, size = n_batch // 2, 4, 2
    dma = pltpu.SemaphoreType.DMA
    return pl.pallas_call(
        functools.partial(dispatch_kernel, half, pitch),
        out_shape=pltpu.VMEM((dim // 128, n_slots // 4 * pitch, 128), F32),
        in_specs=[pl.BlockSpec(memory_space=pl.ANY), pl.BlockSpec(memory_space=pltpu.VMEM), pl.BlockSpec(memory_space=pltpu.SMEM), pl.BlockSpec(memory_space=pltpu.SMEM)],
        out_specs=pl.BlockSpec(memory_space=pltpu.VMEM),
        scratch_shapes=[
            pltpu.VMEM((n_slots, dim), BF16),
            pltpu.VMEM((ring, tok, dim), BF16),
            pltpu.VMEM((half, n_slots, dim), BF16),
            pltpu.VMEM((half, n_slots // 2, dim), BF16),
            pltpu.VMEM((half, n_slots // 4, dim), BF16),
            pltpu.VMEM((half, n_slots // 4, dim), BF16),
            pltpu.VMEM((half, n_slots // 4, dim), BF16),
            pltpu.VMEM((2, half, 1, n_slots // 2), F32),
            pltpu.VMEM((half, 1, n_slots // 2), F32),
            pltpu.VMEM((half, 1, n_slots // 2), F32),
            pltpu.VMEM((half, 1, n_slots // 2), F32),
            pltpu.VMEM((size, n_slots // 2, 8), F32),
            dma((ring,)),
        ] + [dma((half // size,))] * 10,
        compiler_params=pltpu.CompilerParams(collective_id=0, has_side_effects=True, vmem_limit_bytes=20 << 20),
        name="dispatch",
    )(tokens, phi, lengths, g)


def expert_kernel(n_group, n_chunk, pitch, x_hbm, phi_ref, len_ref, g_ref, xs_ref, win_hbm, wout_hbm, c_ref, ys_hbm, v_ref, xbuf, wi, wo, acc, ysend, yrecv, x_sem, wi_sem, wo_sem, y_s, y_r, x_s, x_r, d_s, d_r, r_s, r_r, l_s):
    n_batch, tok, dim = x_hbm.shape
    n_expert = win_hbm.shape[0]
    group = n_expert // n_group
    sub = n_batch // n_chunk
    kg = g_ref[0] * LOG2E
    y, x, core, s, partner, across_x, across_y = place()
    x_ring, w_ring = xbuf.shape[0], wi.shape[0]
    n_pair = n_expert // 2
    n_q = n_group * n_chunk

    def load_x(b):
        slot = lax.rem(b, x_ring)
        return pltpu.make_async_copy(x_hbm.at[b], xbuf.at[slot], x_sem.at[slot])

    def load_w(p):
        slot = lax.rem(p, w_ring)
        return (
            pltpu.make_async_copy(win_hbm.at[pl.ds(2 * p, 2)], wi.at[slot], wi_sem.at[slot]),
            pltpu.make_async_copy(wout_hbm.at[pl.ds(2 * p, 2)], wo.at[slot], wo_sem.at[slot]),
        )

    def home(q, on_core, on_x):
        g, bq = q // n_chunk, lax.rem(q, n_chunk)
        slot0 = pl.multiple_of((on_x * 2 + on_core) * n_expert + g * group, group)
        return ys_hbm.at[pl.ds(bq * sub, sub), pl.ds(slot0, group)]

    def y_copy(q):
        return remote(ysend.at[q], yrecv.at[q], y_s.at[q], y_r.at[q], across_y)

    def x_copy(q):
        return remote(yrecv.at[q], home(q, core, x), x_s.at[q], x_r.at[q], across_x)

    def x_arrival(q):
        return remote(yrecv.at[q], home(q, core, 1 - x), x_s.at[q], x_r.at[q], across_x)

    def core_copy(q):
        return remote(yrecv.at[q], home(q, core, x), d_s.at[q], d_r.at[q], partner)

    def core_arrival(q):
        return remote(yrecv.at[q], home(q, 1 - core, x), d_s.at[q], d_r.at[q], partner)

    def relay(q):
        return remote(home(q, core, 1 - x), home(q, core, 1 - x), r_s.at[q], r_r.at[q], partner)

    def relay_arrival(q):
        return remote(home(q, 1 - core, 1 - x), home(q, 1 - core, 1 - x), r_s.at[q], r_r.at[q], partner)

    def local_copy(q):
        return pltpu.make_async_copy(yrecv.at[q], home(q, core, x), l_s.at[q])

    for p in range(w_ring):
        for copy in load_w(p):
            copy.start()
    for b in range(x_ring):
        load_x(b).start()
    v_ref[...] = unit_columns(phi_ref[...]).astype(BF16)
    greet((partner, across_x, across_y))

    def expert_pair(p, carry):
        for copy in load_w(p):
            copy.wait()
        slot = lax.rem(p, w_ring)
        for j in range(2):
            e = 2 * p + j
            rows = gather_rows(xs_ref, pl.ds(pl.multiple_of(e * pitch, 8), n_batch)).astype(BF16)
            hidden = jnp.dot(rows, wi[slot, j], preferred_element_type=F32)
            hidden = (0.5 * hidden * (1.0 + lax.erf(hidden * math.sqrt(0.5)))).astype(BF16)
            out = jnp.dot(hidden, wo[slot, j], preferred_element_type=F32)
            scatter_rows(acc, lax.rem(e, group), group, out)

        @pl.when(p + w_ring < n_pair)
        def _():
            for copy in load_w(p + w_ring):
                copy.start()

        return carry

    def mix_block(b, carry):
        load_x(b).wait()
        slot = lax.rem(b, x_ring)
        xv = xbuf[slot]
        xf = xv.astype(F32)
        scale = lax.rsqrt(jnp.sum(xf * xf, axis=1, keepdims=True) + NORM_EPS) * kg
        logits = jnp.dot(xv, v_ref[...], preferred_element_type=F32) * scale
        weights = jnp.exp2(logits - jnp.max(logits, axis=1, keepdims=True))
        valid = lax.broadcasted_iota(jnp.int32, (tok, 1), 0) < len_ref[b] - s * tok
        inverse = jnp.where(valid, 1.0 / jnp.sum(weights, axis=1, keepdims=True), 0.0)
        c_ref[b] = (weights * inverse).astype(BF16)

        @pl.when(b + x_ring < n_batch)
        def _():
            load_x(b + x_ring).start()

        return carry

    per = n_expert // n_q
    lag = n_chunk + 1
    early, late = 3, 5

    def mix_start(t):
        first = jnp.maximum(t - n_chunk, 0) * early
        return jnp.minimum(jnp.where(t < n_q, first, (n_q - n_chunk) * early + (t - n_q) * late), n_batch)

    def step(t, carry):
        @pl.when(t < n_q)
        def _():
            lax.fori_loop(t * (per // 2), (t + 1) * (per // 2), expert_pair, 0)

        @pl.when((t < n_q) & (lax.rem(t, n_chunk) == n_chunk - 1))
        def _():
            g = t // n_chunk

            def pack(bq, carry):
                rows = gather_rows(acc, pl.ds(pl.multiple_of(bq * sub * group, sub * group), sub * group))
                q = g * n_chunk + bq
                ysend[q] = rows.reshape(sub, group, dim).astype(BF16)
                y_copy(q).start()
                return carry

            lax.fori_loop(0, n_chunk, pack, 0)

        lax.fori_loop(mix_start(t), mix_start(t + 1), mix_block, 0)

        @pl.when((t >= lag) & (t < n_q + lag))
        def _():
            q = t - lag
            y_copy(q).wait_recv()

            def add(i, carry):
                some = pl.ds(i * 8, 8)
                yrecv[q, some] = (ysend[q, some].astype(F32) + yrecv[q, some].astype(F32)).astype(BF16)
                return carry

            lax.fori_loop(0, sub // 8, add, 0)
            x_copy(q).start()
            core_copy(q).start()
            local_copy(q).start()

        @pl.when(t >= lag + 2)
        def _():
            q = t - lag - 2
            x_arrival(q).wait_recv()
            relay(q).start()

        return carry

    lax.fori_loop(0, n_q + lag + 2, step, 0)

    def drain(q, carry):
        core_arrival(q).wait_recv()
        relay_arrival(q).wait_recv()
        y_copy(q).wait_send()
        x_copy(q).wait_send()
        core_copy(q).wait_send()
        relay(q).wait_send()
        local_copy(q).wait()
        return carry

    lax.fori_loop(0, n_q, drain, 0)


def experts(tokens, phi, lengths, g, xs, w_in, w_out, pitch):
    n_batch, tok, dim = tokens.shape
    n_slots = phi.shape[1]
    n_expert, _, hid = w_in.shape
    n_group, n_chunk = 8, 2
    group, sub = n_expert // n_group, n_batch // n_chunk
    n_q = n_group * n_chunk
    x_ring, w_ring = 3, 3
    dma = pltpu.SemaphoreType.DMA
    vmem, smem, anym = pl.BlockSpec(memory_space=pltpu.VMEM), pl.BlockSpec(memory_space=pltpu.SMEM), pl.BlockSpec(memory_space=pl.ANY)
    return pl.pallas_call(
        functools.partial(expert_kernel, n_group, n_chunk, pitch),
        out_shape=(pltpu.VMEM((n_batch, tok, n_slots), BF16), jax.ShapeDtypeStruct((n_batch, n_slots, dim), BF16)),
        in_specs=[anym, vmem, smem, smem, vmem, anym, anym],
        out_specs=(vmem, anym),
        scratch_shapes=[
            pltpu.VMEM((dim, n_slots), BF16),
            pltpu.VMEM((x_ring, tok, dim), BF16),
            pltpu.VMEM((w_ring, 2, dim, hid), BF16),
            pltpu.VMEM((w_ring, 2, hid, dim), BF16),
            pltpu.VMEM((dim // 128, group * n_batch, 128), F32),
            pltpu.VMEM((n_q, sub, group, dim), BF16),
            pltpu.VMEM((n_q, sub, group, dim), BF16),
            dma((x_ring,)),
            dma((w_ring,)),
            dma((w_ring,)),
        ] + [dma((n_q,))] * 9,
        compiler_params=pltpu.CompilerParams(collective_id=1, has_side_effects=True, vmem_limit_bytes=18 << 20),
        name="experts",
    )(tokens, phi, lengths, g, xs, w_in, w_out)


def combine_kernel(c_ref, ys_hbm, y_hbm, ys, out, ys_sem, y_sem):
    n_batch, ring = c_ref.shape[0], out.shape[0]
    depth, step = ys.shape[0], ys.shape[1]
    n_group = n_batch // step

    def load(i):
        slot = lax.rem(i, depth)
        return pltpu.make_async_copy(ys_hbm.at[pl.ds(i * step, step)], ys.at[slot], ys_sem.at[slot])

    def store(b):
        slot = lax.rem(b, ring)
        return pltpu.make_async_copy(out.at[slot], y_hbm.at[b], y_sem.at[slot])

    for i in range(depth):
        load(i).start()

    def group(i, carry):
        load(i).wait()

        @pl.when(i * step >= ring)
        def _():
            for j in range(step):
                store(i * step + j - ring).wait()

        for j in range(step):
            b = i * step + j
            out[lax.rem(b, ring)] = jnp.dot(c_ref[b], ys[lax.rem(i, depth), j], preferred_element_type=F32).astype(BF16)
        for j in range(step):
            store(i * step + j).start()

        @pl.when(i + depth < n_group)
        def _():
            load(i + depth).start()

        return carry

    lax.fori_loop(0, n_group, group, 0)

    def drain(b, carry):
        store(b).wait()
        return carry

    lax.fori_loop(n_batch - ring, n_batch, drain, 0)


def combine(c, ys):
    n_batch, tok, n_slots = c.shape
    dim = ys.shape[2]
    step, depth, ring = 4, 4, 16
    return pl.pallas_call(
        combine_kernel,
        out_shape=jax.ShapeDtypeStruct((n_batch, tok, dim), BF16),
        in_specs=[pl.BlockSpec(memory_space=pltpu.VMEM), pl.BlockSpec(memory_space=pl.ANY)],
        out_specs=pl.BlockSpec(memory_space=pl.ANY),
        scratch_shapes=[
            pltpu.VMEM((depth, step, n_slots, dim), BF16),
            pltpu.VMEM((ring, tok, dim), BF16),
            pltpu.SemaphoreType.DMA((depth,)),
            pltpu.SemaphoreType.DMA((ring,)),
        ],
        compiler_params=pltpu.CompilerParams(vmem_limit_bytes=20 << 20),
        name="combine",
    )(c, ys)


def solution(mesh):
    def local_layer(tokens, lengths, slot_params, logit_scale, w_in, w_out):
        pitch = tokens.shape[0] + 8
        g = logit_scale.reshape(1)
        xs = dispatch(tokens, slot_params, lengths, g, pitch)
        c, ys = experts(tokens, slot_params, lengths, g, pltpu.with_memory_space_constraint(xs, pltpu.VMEM), w_in, w_out, pitch)
        return combine(pltpu.with_memory_space_constraint(c, pltpu.VMEM), ys)

    return jax.shard_map(local_layer, mesh=mesh, in_specs=(P("data", "seq", None), P("data"), P(), P(), P("seq", None, "model"), P("seq", "model", None)), out_specs=P("data", "seq", None), check_vma=False)
```

```python
import functools
import math
import jax
import jax.numpy as jnp
from jax import lax
from jax.experimental import pallas as pl
from jax.experimental.pallas import tpu as pltpu
from jax.sharding import PartitionSpec as P

NORM_EPS = 1e-6
LOG2E = math.log2(math.e)
MASKED = -1e30
MESH = pl.DeviceIdType.MESH
F32, BF16 = jnp.float32, jnp.bfloat16
NT = (((1,), (1,)), ((), ()))


def unit_columns(values):
    v32 = values.astype(F32)
    return v32 * lax.rsqrt(jnp.sum(v32 * v32, axis=0, keepdims=True) + NORM_EPS)


def place():
    y, s = lax.axis_index("model"), lax.axis_index("seq")
    x, core = s // 2, lax.rem(s, 2)
    partner = (0, y, x * 2 + 1 - core)
    across_x = (0, y, (1 - x) * 2 + core)
    across_y = (0, 1 - y, s)
    return y, x, core, s, partner, across_x, across_y


def greet(devices):
    barrier = pltpu.get_barrier_semaphore()
    for device in devices:
        pl.semaphore_signal(barrier, inc=1, device_id=device, device_id_type=MESH)
    pl.semaphore_wait(barrier, len(devices))


def remote(src, dst, send, recv, device):
    return pltpu.make_async_remote_copy(src_ref=src, dst_ref=dst, send_sem=send, recv_sem=recv, device_id=device, device_id_type=MESH)


def small_copies(phi_hbm, phi_ref, len_hbm, len_ref, sem):
    return pltpu.make_async_copy(phi_hbm, phi_ref, sem.at[0]), pltpu.make_async_copy(len_hbm, len_ref, sem.at[1])


def merge_weights(a, b):
    top = jnp.maximum(a, b)
    ea, eb = jnp.exp2(a - top), jnp.exp2(b - top)
    total = ea + eb
    row = lax.broadcasted_iota(jnp.int32, (8, a.shape[1]), 0)
    weights = jnp.where(row == 0, ea, eb) * (1.0 / total)
    return jnp.transpose(weights), top + jnp.log2(total)


def scatter_rows(acc, first, stride, rows):
    for j in range(acc.shape[0]):
        acc[j, pl.ds(first, rows.shape[0], stride=stride), :] = rows[:, j * 128 : (j + 1) * 128]


def gather_rows(acc, rows):
    return jnp.concatenate([acc[j, rows, :] for j in range(acc.shape[0])], axis=1)


def dispatch_kernel(half, pitch, x_hbm, phi_hbm, len_hbm, g_ref, xs_ref, phi_ref, len_ref, vt_ref, xbuf, part, mid, xpart, own, yown, lse, dlse, mlse, xlse, wcol, small_sem, in_sem, d_s, d_r, dl_s, dl_r, x_s, x_r, xl_s, xl_r, y_s, y_r):
    size = part.shape[0] // d_s.shape[0]
    n_step = half // size
    tok, n_slots, dim = xbuf.shape[1], vt_ref.shape[0], xbuf.shape[2]
    core_slots, dev_slots = n_slots // 2, n_slots // 4
    y, x, core, s, partner, across_x, across_y = place()
    base = y * half
    ring = xbuf.shape[0]
    kg = g_ref[0] * LOG2E

    def load(i):
        slot = lax.rem(i, ring)
        return pltpu.make_async_copy(x_hbm.at[base + i], xbuf.at[slot], in_sem.at[slot])

    def core_copy(u):
        rows, some = pl.ds(pl.multiple_of((1 - core) * core_slots, core_slots), core_slots), pl.ds(u * size, size)
        return remote(part.at[some, rows], mid.at[some], d_s.at[u], d_r.at[u], partner)

    def core_lse(u):
        some = pl.ds(u * size, size)
        return remote(lse.at[1 - core, some], dlse.at[some], dl_s.at[u], dl_r.at[u], partner)

    def x_copy(u):
        rows, some = pl.ds(pl.multiple_of((1 - x) * dev_slots, dev_slots), dev_slots), pl.ds(u * size, size)
        return remote(mid.at[some, rows], xpart.at[some], x_s.at[u], x_r.at[u], across_x)

    def x_lse(u):
        some = pl.ds(u * size, size)
        return remote(mlse.at[some], xlse.at[some], xl_s.at[u], xl_r.at[u], across_x)

    def y_copy(u):
        some = pl.ds(u * size, size)
        return remote(own.at[some], yown.at[some], y_s.at[u], y_r.at[u], across_y)

    small = small_copies(phi_hbm, phi_ref, len_hbm, len_ref, small_sem)
    for copy in small:
        copy.start()
    for i in range(size):
        load(i).start()
    for copy in small:
        copy.wait()
    v_rows = jnp.transpose(unit_columns(phi_ref[...]))
    for j, block in enumerate((0, 2, 1, 3)):
        vt_ref[j * dev_slots : (j + 1) * dev_slots] = v_rows[block * dev_slots : (block + 1) * dev_slots].astype(BF16)
    greet((partner, across_x, across_y))
    for i in range(size, ring):
        load(i).start()

    def local_mean(i):
        xv = xbuf[lax.rem(i, ring)]
        xf = xv.astype(F32)
        square = jnp.sum(xf * xf, axis=1, keepdims=True)
        square_row = jnp.transpose(jnp.broadcast_to(square, (tok, 128)))[0:1]
        scale_row = lax.rsqrt(square_row + NORM_EPS) * kg
        logits = lax.dot_general(vt_ref[...], xv, NT, preferred_element_type=F32) * scale_row
        lane = lax.broadcasted_iota(jnp.int32, (1, tok), 1)
        masked = jnp.where(lane < len_ref[base + i] - s * tok, logits, MASKED)
        top = jnp.max(masked, axis=1, keepdims=True)
        weights = jnp.exp2(masked - top)
        total = jnp.sum(weights, axis=1, keepdims=True)
        mean = jnp.dot(weights.astype(BF16), xv, preferred_element_type=F32) * (1.0 / total)
        part[i] = mean.astype(BF16)
        first = lax.broadcasted_iota(jnp.int32, (n_slots, 128), 1) == 0
        rows = jnp.transpose(jnp.where(first, top, total))
        row = rows[0:1] + jnp.log2(rows[1:2])
        lse[0, i] = row[:, :core_slots]
        lse[1, i] = row[:, core_slots:]

    def step(u, carry):
        @pl.when(u < n_step)
        def _():
            for j in range(size):
                load(u * size + j).wait()
            for j in range(size):
                local_mean(u * size + j)
            core_copy(u).start()
            core_lse(u).start()

            @pl.when(u * size + ring < half)
            def _():
                for j in range(size):
                    load(u * size + j + ring).start()

        def core_wait():
            core_copy(u - 1).wait_recv()
            core_lse(u - 1).wait_recv()

        def core_merge():
            rows = pl.ds(pl.multiple_of(core * core_slots, core_slots), core_slots)
            for j in range(size):
                k = (u - 1) * size + j
                cols, row = merge_weights(lse[core, k], dlse[k])
                merged = cols[:, 0:1] * part[k, rows].astype(F32) + cols[:, 1:2] * mid[k].astype(F32)
                mid[k] = merged.astype(BF16)
                mlse[k] = row

        def core_send():
            x_copy(u - 1).start()
            x_lse(u - 1).start()

        def x_wait():
            x_copy(u - 3).wait_recv()
            x_lse(u - 3).wait_recv()

        def x_merge():
            rows = pl.ds(pl.multiple_of(x * dev_slots, dev_slots), dev_slots)
            for j in range(size):
                k = (u - 3) * size + j
                cols, _ = merge_weights(mlse[k], xlse[k])
                wcol[j] = cols
                mine = wcol[j, rows, :]
                merged = mine[:, 0:1] * mid[k, rows].astype(F32) + mine[:, 1:2] * xpart[k].astype(F32)
                own[k] = merged.astype(BF16)
                scatter_rows(xs_ref, base + k, pitch, merged)

        def y_place():
            for j in range(size):
                k = (u - 5) * size + j
                scatter_rows(xs_ref, (1 - y) * half + k, pitch, yown[k].astype(F32))

        steady = (u >= 5) & (u <= n_step)

        @pl.when(steady)
        def _():
            core_wait()
            x_wait()
            y_copy(u - 5).wait_recv()
            core_merge()
            x_merge()
            y_place()
            core_send()
            y_copy(u - 3).start()

        @pl.when((u >= 1) & (u < 5))
        def _():
            core_wait()
            core_merge()
            core_send()

        @pl.when((u >= 3) & (u < n_step + 3) & jnp.logical_not(steady))
        def _():
            x_wait()
            x_merge()
            y_copy(u - 3).start()

        @pl.when(u > n_step)
        def _():
            y_copy(u - 5).wait_recv()
            y_place()

        return carry

    lax.fori_loop(0, n_step + 5, step, 0)

    def drain(u, carry):
        core_copy(u).wait_send()
        core_lse(u).wait_send()
        x_copy(u).wait_send()
        x_lse(u).wait_send()
        y_copy(u).wait_send()
        return carry

    lax.fori_loop(0, n_step, drain, 0)


def dispatch(tokens, phi, lengths, g, pitch):
    n_batch, tok, dim = tokens.shape
    n_slots = phi.shape[1]
    half, ring, size = n_batch // 2, 4, 2
    dma = pltpu.SemaphoreType.DMA
    return pl.pallas_call(
        functools.partial(dispatch_kernel, half, pitch),
        out_shape=pltpu.VMEM((dim // 128, n_slots // 4 * pitch, 128), F32),
        in_specs=[pl.BlockSpec(memory_space=pl.ANY)] * 3 + [pl.BlockSpec(memory_space=pltpu.SMEM)],
        out_specs=pl.BlockSpec(memory_space=pltpu.VMEM),
        scratch_shapes=[
            pltpu.VMEM((dim, n_slots), BF16),
            pltpu.SMEM((n_batch,), jnp.int32),
            pltpu.VMEM((n_slots, dim), BF16),
            pltpu.VMEM((ring, tok, dim), BF16),
            pltpu.VMEM((half, n_slots, dim), BF16),
            pltpu.VMEM((half, n_slots // 2, dim), BF16),
            pltpu.VMEM((half, n_slots // 4, dim), BF16),
            pltpu.VMEM((half, n_slots // 4, dim), BF16),
            pltpu.VMEM((half, n_slots // 4, dim), BF16),
            pltpu.VMEM((2, half, 1, n_slots // 2), F32),
            pltpu.VMEM((half, 1, n_slots // 2), F32),
            pltpu.VMEM((half, 1, n_slots // 2), F32),
            pltpu.VMEM((half, 1, n_slots // 2), F32),
            pltpu.VMEM((size, n_slots // 2, 8), F32),
            dma((2,)),
            dma((ring,)),
        ] + [dma((half // size,))] * 10,
        compiler_params=pltpu.CompilerParams(collective_id=0, has_side_effects=True, vmem_limit_bytes=20 << 20),
        name="dispatch",
    )(tokens, phi, lengths, g)


def expert_kernel(n_group, n_chunk, pitch, x_hbm, phi_hbm, len_hbm, g_ref, xs_ref, win_hbm, wout_hbm, c_ref, ys_hbm, phi_ref, len_ref, v_ref, xbuf, wi, wo, acc, ysend, yrecv, small_sem, x_sem, wi_sem, wo_sem, y_s, y_r, x_s, x_r, d_s, d_r, r_s, r_r, l_s, f_s, f_r):
    n_batch, tok, dim = x_hbm.shape
    n_expert = win_hbm.shape[0]
    group = n_expert // n_group
    sub = n_batch // n_chunk
    kg = g_ref[0] * LOG2E
    y, x, core, s, partner, across_x, across_y = place()
    x_ring, w_ring, y_ring = xbuf.shape[0], wi.shape[0], ysend.shape[0]
    n_pair = n_expert // 2
    n_q = n_group * n_chunk

    def load_x(b):
        slot = lax.rem(b, x_ring)
        return pltpu.make_async_copy(x_hbm.at[b], xbuf.at[slot], x_sem.at[slot])

    def load_w(p):
        slot = lax.rem(p, w_ring)
        return (
            pltpu.make_async_copy(win_hbm.at[pl.ds(2 * p, 2)], wi.at[slot], wi_sem.at[slot]),
            pltpu.make_async_copy(wout_hbm.at[pl.ds(2 * p, 2)], wo.at[slot], wo_sem.at[slot]),
        )

    def home(q, on_core, on_x):
        g, bq = q // n_chunk, lax.rem(q, n_chunk)
        slot0 = pl.multiple_of((on_x * 2 + on_core) * n_expert + g * group, group)
        return ys_hbm.at[pl.ds(bq * sub, sub), pl.ds(slot0, group)]

    def y_copy(q):
        return remote(ysend.at[lax.rem(q, y_ring)], yrecv.at[q], y_s.at[q], y_r.at[q], across_y)

    def first_copy(p, bq):
        some, k = pl.ds(p * (sub // 4), sub // 4), p * n_chunk + bq
        return remote(ysend.at[bq, some], yrecv.at[bq, some], f_s.at[k], f_r.at[k], across_y)

    def x_copy(q):
        return remote(yrecv.at[q], home(q, core, x), x_s.at[q], x_r.at[q], across_x)

    def x_arrival(q):
        return remote(yrecv.at[q], home(q, core, 1 - x), x_s.at[q], x_r.at[q], across_x)

    def core_copy(q):
        return remote(yrecv.at[q], home(q, core, x), d_s.at[q], d_r.at[q], partner)

    def core_arrival(q):
        return remote(yrecv.at[q], home(q, 1 - core, x), d_s.at[q], d_r.at[q], partner)

    def relay(q):
        return remote(home(q, core, 1 - x), home(q, core, 1 - x), r_s.at[q], r_r.at[q], partner)

    def relay_arrival(q):
        return remote(home(q, 1 - core, 1 - x), home(q, 1 - core, 1 - x), r_s.at[q], r_r.at[q], partner)

    def local_copy(q):
        return pltpu.make_async_copy(yrecv.at[q], home(q, core, x), l_s.at[q])

    small = small_copies(phi_hbm, phi_ref, len_hbm, len_ref, small_sem)
    for copy in (*small, *load_w(0)):
        copy.start()
    for copy in small:
        copy.wait()
    v_ref[...] = unit_columns(phi_ref[...]).astype(BF16)
    greet((partner, across_x, across_y))
    for p in range(1, w_ring):
        for copy in load_w(p):
            copy.start()

    def expert_pair(p, carry):
        for copy in load_w(p):
            copy.wait()
        slot = lax.rem(p, w_ring)
        for j in range(2):
            e = 2 * p + j
            rows = gather_rows(xs_ref, pl.ds(pl.multiple_of(e * pitch, 8), n_batch)).astype(BF16)
            hidden = jnp.dot(rows, wi[slot, j], preferred_element_type=F32)
            hidden = (0.5 * hidden * (1.0 + lax.erf(hidden * math.sqrt(0.5)))).astype(BF16)
            out = jnp.dot(hidden, wo[slot, j], preferred_element_type=F32)
            g, first = e // group, pl.multiple_of(lax.rem(e, group) * (sub // 8), sub // 8)
            for bq in range(n_chunk):
                piece = out[bq * sub : (bq + 1) * sub].astype(BF16)
                ysend[lax.rem(g * n_chunk + bq, y_ring), pl.ds(first, sub // 8)] = piece.reshape(sub // 8, 8, dim)

        @pl.when(p < group // 2)
        def _():
            for bq in range(n_chunk):
                first_copy(p, bq).start()

        @pl.when(p + w_ring < n_pair)
        def _():
            for copy in load_w(p + w_ring):
                copy.start()

        return carry

    def mix_one(b):
        xv = xbuf[lax.rem(b, x_ring)]
        xf = xv.astype(F32)
        scale = lax.rsqrt(jnp.sum(xf * xf, axis=1, keepdims=True) + NORM_EPS) * kg
        logits = jnp.dot(xv, v_ref[...], preferred_element_type=F32) * scale
        weights = jnp.exp2(logits - jnp.max(logits, axis=1, keepdims=True))
        valid = lax.broadcasted_iota(jnp.int32, (tok, 1), 0) < len_ref[b] - s * tok
        inverse = jnp.where(valid, 1.0 / jnp.sum(weights, axis=1, keepdims=True), 0.0)
        c_ref[b] = (weights * inverse).astype(BF16)

    def mix_pair(m, carry):
        for j in range(2):
            load_x(2 * m + j).wait()
        for j in range(2):
            mix_one(2 * m + j)

        @pl.when(2 * m + x_ring < n_batch)
        def _():
            for j in range(2):
                load_x(2 * m + j + x_ring).start()

        return carry

    per = n_expert // n_q
    lag = 3
    n_mix = n_batch // 2
    early = 20

    def mix_start(t):
        first = jnp.maximum(t - n_chunk, 0) * early // (n_q - n_chunk)
        rest = early + (t - n_q) * (n_mix - early) // (lag + 3)
        return jnp.where(t < n_q, first, rest)

    def step(t, carry):
        @pl.when(t < n_q)
        def _():
            lax.fori_loop(t * (per // 2), (t + 1) * (per // 2), expert_pair, 0)

        @pl.when((t >= n_chunk) & (t < n_q) & (lax.rem(t, n_chunk) == n_chunk - 1))
        def _():
            for bq in range(n_chunk):
                y_copy(t - n_chunk + 1 + bq).start()

        @pl.when(t == 0)
        def _():
            for b in range(x_ring):
                load_x(b).start()

        lax.fori_loop(mix_start(t), mix_start(t + 1), mix_pair, 0)

        @pl.when((t >= lag) & (t < n_q + lag))
        def _():
            q = t - lag

            @pl.when(q < n_chunk)
            def _():
                for p in range(group // 2):
                    first_copy(p, q).wait_recv()

            @pl.when(q >= n_chunk)
            def _():
                y_copy(q).wait_recv()

            total = ysend[lax.rem(q, y_ring)].astype(F32) + yrecv[q].astype(F32)
            total = total.reshape(group * sub, dim)
            for e in range(group):
                scatter_rows(acc, e, group, total[e * sub : (e + 1) * sub])
            yrecv[q] = gather_rows(acc, pl.ds(0, group * sub)).reshape(sub, group, dim).astype(BF16)
            x_copy(q).start()
            core_copy(q).start()
            local_copy(q).start()

            @pl.when(q < n_chunk)
            def _():
                for p in range(group // 2):
                    first_copy(p, q).wait_send()

            @pl.when(q >= n_chunk)
            def _():
                y_copy(q).wait_send()

        @pl.when(t >= lag + 3)
        def _():
            q = t - lag - 3
            x_arrival(q).wait_recv()
            relay(q).start()

        return carry

    lax.fori_loop(0, n_q + lag + 3, step, 0)

    def drain(q, carry):
        core_arrival(q).wait_recv()
        relay_arrival(q).wait_recv()
        x_copy(q).wait_send()
        core_copy(q).wait_send()
        relay(q).wait_send()
        local_copy(q).wait()
        return carry

    lax.fori_loop(0, n_q, drain, 0)


def experts(tokens, phi, lengths, g, xs, w_in, w_out, pitch):
    n_batch, tok, dim = tokens.shape
    n_slots = phi.shape[1]
    n_expert, _, hid = w_in.shape
    n_group, n_chunk = 8, 2
    group, sub = n_expert // n_group, n_batch // n_chunk
    n_q = n_group * n_chunk
    x_ring, w_ring = 4, 3
    dma = pltpu.SemaphoreType.DMA
    vmem, smem, anym = pl.BlockSpec(memory_space=pltpu.VMEM), pl.BlockSpec(memory_space=pltpu.SMEM), pl.BlockSpec(memory_space=pl.ANY)
    return pl.pallas_call(
        functools.partial(expert_kernel, n_group, n_chunk, pitch),
        out_shape=(pltpu.VMEM((n_batch, tok, n_slots), BF16), jax.ShapeDtypeStruct((n_batch, n_slots, dim), BF16)),
        in_specs=[anym, anym, anym, smem, vmem, anym, anym],
        out_specs=(vmem, anym),
        scratch_shapes=[
            pltpu.VMEM((dim, n_slots), BF16),
            pltpu.SMEM((n_batch,), jnp.int32),
            pltpu.VMEM((dim, n_slots), BF16),
            pltpu.VMEM((x_ring, tok, dim), BF16),
            pltpu.VMEM((w_ring, 2, dim, hid), BF16),
            pltpu.VMEM((w_ring, 2, hid, dim), BF16),
            pltpu.VMEM((dim // 128, group * sub, 128), F32),
            pltpu.VMEM((n_q // 2, sub, group, dim), BF16),
            pltpu.VMEM((n_q, sub, group, dim), BF16),
            dma((2,)),
            dma((x_ring,)),
            dma((w_ring,)),
            dma((w_ring,)),
        ] + [dma((n_q,))] * 9 + [dma((group // 2 * n_chunk,))] * 2,
        compiler_params=pltpu.CompilerParams(collective_id=1, has_side_effects=True, vmem_limit_bytes=18 << 20),
        name="experts",
    )(tokens, phi, lengths, g, xs, w_in, w_out)


def combine_kernel(c_ref, ys_hbm, y_hbm, ys, out, ys_sem, y_sem):
    n_batch, ring = c_ref.shape[0], out.shape[0]
    depth, step = ys.shape[0], ys.shape[1]
    n_group = n_batch // step

    def load(i):
        slot = lax.rem(i, depth)
        return pltpu.make_async_copy(ys_hbm.at[pl.ds(i * step, step)], ys.at[slot], ys_sem.at[slot])

    def store(b):
        slot = lax.rem(b, ring)
        return pltpu.make_async_copy(out.at[slot], y_hbm.at[b], y_sem.at[slot])

    for i in range(depth):
        load(i).start()

    def group(i, carry):
        load(i).wait()

        @pl.when(i * step >= ring)
        def _():
            for j in range(step):
                store(i * step + j - ring).wait()

        for j in range(step):
            b = i * step + j
            out[lax.rem(b, ring)] = jnp.dot(c_ref[b], ys[lax.rem(i, depth), j], preferred_element_type=F32).astype(BF16)
        for j in range(step):
            store(i * step + j).start()

        @pl.when(i + depth < n_group)
        def _():
            load(i + depth).start()

        return carry

    lax.fori_loop(0, n_group, group, 0)

    def drain(b, carry):
        store(b).wait()
        return carry

    lax.fori_loop(n_batch - ring, n_batch, drain, 0)


def combine(c, ys):
    n_batch, tok, n_slots = c.shape
    dim = ys.shape[2]
    step, depth, ring = 4, 4, 16
    return pl.pallas_call(
        combine_kernel,
        out_shape=jax.ShapeDtypeStruct((n_batch, tok, dim), BF16),
        in_specs=[pl.BlockSpec(memory_space=pltpu.VMEM), pl.BlockSpec(memory_space=pl.ANY)],
        out_specs=pl.BlockSpec(memory_space=pl.ANY),
        scratch_shapes=[
            pltpu.VMEM((depth, step, n_slots, dim), BF16),
            pltpu.VMEM((ring, tok, dim), BF16),
            pltpu.SemaphoreType.DMA((depth,)),
            pltpu.SemaphoreType.DMA((ring,)),
        ],
        compiler_params=pltpu.CompilerParams(vmem_limit_bytes=20 << 20),
        name="combine",
    )(c, ys)


def solution(mesh):
    def local_layer(tokens, lengths, slot_params, logit_scale, w_in, w_out):
        pitch = tokens.shape[0] + 8
        g = logit_scale.reshape(1)
        phi, lens = (pltpu.with_memory_space_constraint(a, pltpu.HBM) for a in (slot_params, lengths))
        xs = dispatch(tokens, phi, lens, g, pitch)
        c, ys = experts(tokens, phi, lens, g, pltpu.with_memory_space_constraint(xs, pltpu.VMEM), w_in, w_out, pitch)
        return combine(pltpu.with_memory_space_constraint(c, pltpu.VMEM), ys)

    return jax.shard_map(local_layer, mesh=mesh, in_specs=(P("data", "seq", None), P("data"), P(), P(), P("seq", None, "model"), P("seq", "model", None)), out_specs=P("data", "seq", None), check_vma=False)
```

```python
import functools
import math
import jax
import jax.numpy as jnp
from jax import lax
from jax.experimental import pallas as pl
from jax.experimental.pallas import tpu as pltpu
from jax.sharding import PartitionSpec as P

NORM_EPS = 1e-6
LOG2E = math.log2(math.e)
MASKED = -1e30
MESH = pl.DeviceIdType.MESH
F32, BF16 = jnp.float32, jnp.bfloat16
NT = (((1,), (1,)), ((), ()))


def unit_columns(values):
    v32 = values.astype(F32)
    return v32 * lax.rsqrt(jnp.sum(v32 * v32, axis=0, keepdims=True) + NORM_EPS)


def place():
    y, s = lax.axis_index("model"), lax.axis_index("seq")
    x, core = s // 2, lax.rem(s, 2)
    partner = (0, y, x * 2 + 1 - core)
    across_x = (0, y, (1 - x) * 2 + core)
    across_y = (0, 1 - y, s)
    return y, x, core, s, partner, across_x, across_y


def greet(devices):
    barrier = pltpu.get_barrier_semaphore()
    for device in devices:
        pl.semaphore_signal(barrier, inc=1, device_id=device, device_id_type=MESH)
    pl.semaphore_wait(barrier, len(devices))


def remote(src, dst, send, recv, device):
    return pltpu.make_async_remote_copy(src_ref=src, dst_ref=dst, send_sem=send, recv_sem=recv, device_id=device, device_id_type=MESH)


def small_copies(phi_hbm, phi_ref, len_hbm, len_ref, sem):
    return pltpu.make_async_copy(phi_hbm, phi_ref, sem.at[0]), pltpu.make_async_copy(len_hbm, len_ref, sem.at[1])


def merge_weights(a, b):
    top = jnp.maximum(a, b)
    ea, eb = jnp.exp2(a - top), jnp.exp2(b - top)
    total = ea + eb
    row = lax.broadcasted_iota(jnp.int32, (8, a.shape[1]), 0)
    weights = jnp.where(row == 0, ea, eb) * (1.0 / total)
    return jnp.transpose(weights), top + jnp.log2(total)


def scatter_rows(acc, first, stride, rows):
    for j in range(acc.shape[0]):
        acc[j, pl.ds(first, rows.shape[0], stride=stride), :] = rows[:, j * 128 : (j + 1) * 128]


def gather_rows(acc, rows):
    return jnp.concatenate([acc[j, rows, :] for j in range(acc.shape[0])], axis=1)


def dispatch_kernel(half, pitch, x_hbm, phi_hbm, len_hbm, g_ref, xs_ref, phi_ref, len_ref, vt_ref, xbuf, part, mid, xpart, own, yown, lse, dlse, mlse, xlse, wcol, small_sem, in_sem, d_s, d_r, dl_s, dl_r, x_s, x_r, xl_s, xl_r, y_s, y_r):
    size = part.shape[0] // d_s.shape[0]
    n_step = half // size
    tok, n_slots, dim = xbuf.shape[1], vt_ref.shape[0], xbuf.shape[2]
    core_slots, dev_slots = n_slots // 2, n_slots // 4
    y, x, core, s, partner, across_x, across_y = place()
    base = y * half
    ring = xbuf.shape[0]
    kg = g_ref[0] * LOG2E

    def load(i):
        slot = lax.rem(i, ring)
        return pltpu.make_async_copy(x_hbm.at[base + i], xbuf.at[slot], in_sem.at[slot])

    def core_copy(u):
        rows, some = pl.ds(pl.multiple_of((1 - core) * core_slots, core_slots), core_slots), pl.ds(u * size, size)
        return remote(part.at[some, rows], mid.at[some], d_s.at[u], d_r.at[u], partner)

    def core_lse(u):
        some = pl.ds(u * size, size)
        return remote(lse.at[1 - core, some], dlse.at[some], dl_s.at[u], dl_r.at[u], partner)

    def x_copy(u):
        rows, some = pl.ds(pl.multiple_of((1 - x) * dev_slots, dev_slots), dev_slots), pl.ds(u * size, size)
        return remote(mid.at[some, rows], xpart.at[some], x_s.at[u], x_r.at[u], across_x)

    def x_lse(u):
        some = pl.ds(u * size, size)
        return remote(mlse.at[some], xlse.at[some], xl_s.at[u], xl_r.at[u], across_x)

    def y_copy(u):
        some = pl.ds(u * size, size)
        return remote(own.at[some], yown.at[some], y_s.at[u], y_r.at[u], across_y)

    small = small_copies(phi_hbm, phi_ref, len_hbm, len_ref, small_sem)
    for copy in small:
        copy.start()
    for i in range(size):
        load(i).start()
    for copy in small:
        copy.wait()
    v_rows = jnp.transpose(unit_columns(phi_ref[...]))
    for j, block in enumerate((0, 2, 1, 3)):
        vt_ref[j * dev_slots : (j + 1) * dev_slots] = v_rows[block * dev_slots : (block + 1) * dev_slots].astype(BF16)
    greet((partner, across_x, across_y))
    for i in range(size, ring):
        load(i).start()

    def local_mean(i):
        xv = xbuf[lax.rem(i, ring)]
        xf = xv.astype(F32)
        square = jnp.sum(xf * xf, axis=1, keepdims=True)
        square_row = jnp.transpose(jnp.broadcast_to(square, (tok, 128)))[0:1]
        scale_row = lax.rsqrt(square_row + NORM_EPS) * kg
        logits = lax.dot_general(vt_ref[...], xv, NT, preferred_element_type=F32) * scale_row
        lane = lax.broadcasted_iota(jnp.int32, (1, tok), 1)
        masked = jnp.where(lane < len_ref[base + i] - s * tok, logits, MASKED)
        top = jnp.max(masked, axis=1, keepdims=True)
        weights = jnp.exp2(masked - top)
        total = jnp.sum(weights, axis=1, keepdims=True)
        mean = jnp.dot(weights.astype(BF16), xv, preferred_element_type=F32) * (1.0 / total)
        part[i] = mean.astype(BF16)
        first = lax.broadcasted_iota(jnp.int32, (n_slots, 128), 1) == 0
        rows = jnp.transpose(jnp.where(first, top, total))
        row = rows[0:1] + jnp.log2(rows[1:2])
        lse[0, i] = row[:, :core_slots]
        lse[1, i] = row[:, core_slots:]

    def step(u, carry):
        @pl.when(u < n_step)
        def _():
            for j in range(size):
                load(u * size + j).wait()
            for j in range(size):
                local_mean(u * size + j)
            core_copy(u).start()
            core_lse(u).start()

            @pl.when(u * size + ring < half)
            def _():
                for j in range(size):
                    load(u * size + j + ring).start()

        def core_wait():
            core_copy(u - 1).wait_recv()
            core_lse(u - 1).wait_recv()

        def core_merge():
            rows = pl.ds(pl.multiple_of(core * core_slots, core_slots), core_slots)
            for j in range(size):
                k = (u - 1) * size + j
                cols, row = merge_weights(lse[core, k], dlse[k])
                merged = cols[:, 0:1] * part[k, rows].astype(F32) + cols[:, 1:2] * mid[k].astype(F32)
                mid[k] = merged.astype(BF16)
                mlse[k] = row

        def core_send():
            x_copy(u - 1).start()
            x_lse(u - 1).start()

        def x_wait():
            x_copy(u - 3).wait_recv()
            x_lse(u - 3).wait_recv()

        def x_merge():
            rows = pl.ds(pl.multiple_of(x * dev_slots, dev_slots), dev_slots)
            for j in range(size):
                k = (u - 3) * size + j
                cols, _ = merge_weights(mlse[k], xlse[k])
                wcol[j] = cols
                mine = wcol[j, rows, :]
                merged = mine[:, 0:1] * mid[k, rows].astype(F32) + mine[:, 1:2] * xpart[k].astype(F32)
                own[k] = merged.astype(BF16)
                scatter_rows(xs_ref, base + k, pitch, merged)

        def y_place():
            for j in range(size):
                k = (u - 5) * size + j
                scatter_rows(xs_ref, (1 - y) * half + k, pitch, yown[k].astype(F32))

        steady = (u >= 5) & (u <= n_step)

        @pl.when(steady)
        def _():
            core_wait()
            x_wait()
            y_copy(u - 5).wait_recv()
            core_merge()
            x_merge()
            y_place()
            core_send()
            y_copy(u - 3).start()

        @pl.when((u >= 1) & (u < 5))
        def _():
            core_wait()
            core_merge()
            core_send()

        @pl.when((u >= 3) & (u < n_step + 3) & jnp.logical_not(steady))
        def _():
            x_wait()
            x_merge()
            y_copy(u - 3).start()

        @pl.when(u > n_step)
        def _():
            y_copy(u - 5).wait_recv()
            y_place()

        return carry

    lax.fori_loop(0, n_step + 5, step, 0)

    def drain(u, carry):
        core_copy(u).wait_send()
        core_lse(u).wait_send()
        x_copy(u).wait_send()
        x_lse(u).wait_send()
        y_copy(u).wait_send()
        return carry

    lax.fori_loop(0, n_step, drain, 0)


def dispatch(tokens, phi, lengths, g, pitch):
    n_batch, tok, dim = tokens.shape
    n_slots = phi.shape[1]
    half, ring, size = n_batch // 2, 4, 2
    dma = pltpu.SemaphoreType.DMA
    return pl.pallas_call(
        functools.partial(dispatch_kernel, half, pitch),
        out_shape=pltpu.VMEM((dim // 128, n_slots // 4 * pitch, 128), F32),
        in_specs=[pl.BlockSpec(memory_space=pl.ANY)] * 3 + [pl.BlockSpec(memory_space=pltpu.SMEM)],
        out_specs=pl.BlockSpec(memory_space=pltpu.VMEM),
        scratch_shapes=[
            pltpu.VMEM((dim, n_slots), BF16),
            pltpu.SMEM((n_batch,), jnp.int32),
            pltpu.VMEM((n_slots, dim), BF16),
            pltpu.VMEM((ring, tok, dim), BF16),
            pltpu.VMEM((half, n_slots, dim), BF16),
            pltpu.VMEM((half, n_slots // 2, dim), BF16),
            pltpu.VMEM((half, n_slots // 4, dim), BF16),
            pltpu.VMEM((half, n_slots // 4, dim), BF16),
            pltpu.VMEM((half, n_slots // 4, dim), BF16),
            pltpu.VMEM((2, half, 1, n_slots // 2), F32),
            pltpu.VMEM((half, 1, n_slots // 2), F32),
            pltpu.VMEM((half, 1, n_slots // 2), F32),
            pltpu.VMEM((half, 1, n_slots // 2), F32),
            pltpu.VMEM((size, n_slots // 2, 8), F32),
            dma((2,)),
            dma((ring,)),
        ] + [dma((half // size,))] * 10,
        compiler_params=pltpu.CompilerParams(collective_id=0, has_side_effects=True, vmem_limit_bytes=20 << 20),
        name="dispatch",
    )(tokens, phi, lengths, g)


def expert_kernel(n_group, n_chunk, pitch, x_hbm, phi_hbm, len_hbm, g_ref, xs_ref, win_hbm, wout_hbm, c_ref, ys_hbm, phi_ref, len_ref, v_ref, xbuf, wi, wo, acc, ysend, yrecv, small_sem, x_sem, wi_sem, wo_sem, y_s, y_r, x_s, x_r, d_s, d_r, r_s, r_r, l_s, f_s, f_r):
    n_batch, tok, dim = x_hbm.shape
    n_expert = win_hbm.shape[0]
    group = n_expert // n_group
    sub = n_batch // n_chunk
    kg = g_ref[0] * LOG2E
    y, x, core, s, partner, across_x, across_y = place()
    x_ring, w_ring, y_ring = xbuf.shape[0], wi.shape[0], ysend.shape[0]
    n_pair = n_expert // 2
    n_q = n_group * n_chunk

    def load_x(b):
        slot = lax.rem(b, x_ring)
        return pltpu.make_async_copy(x_hbm.at[b], xbuf.at[slot], x_sem.at[slot])

    def load_w(p):
        slot = lax.rem(p, w_ring)
        return (
            pltpu.make_async_copy(win_hbm.at[pl.ds(2 * p, 2)], wi.at[slot], wi_sem.at[slot]),
            pltpu.make_async_copy(wout_hbm.at[pl.ds(2 * p, 2)], wo.at[slot], wo_sem.at[slot]),
        )

    def home(q, on_core, on_x):
        g, bq = q // n_chunk, lax.rem(q, n_chunk)
        slot0 = pl.multiple_of((on_x * 2 + on_core) * n_expert + g * group, group)
        return ys_hbm.at[pl.ds(bq * sub, sub), pl.ds(slot0, group)]

    def y_copy(q):
        return remote(ysend.at[lax.rem(q, y_ring)], yrecv.at[q], y_s.at[q], y_r.at[q], across_y)

    def first_copy(p, bq):
        some, k = pl.ds(p * (sub // 4), sub // 4), p * n_chunk + bq
        return remote(ysend.at[bq, some], yrecv.at[bq, some], f_s.at[k], f_r.at[k], across_y)

    def x_copy(q):
        return remote(yrecv.at[q], home(q, core, x), x_s.at[q], x_r.at[q], across_x)

    def x_arrival(q):
        return remote(yrecv.at[q], home(q, core, 1 - x), x_s.at[q], x_r.at[q], across_x)

    def core_copy(q):
        return remote(yrecv.at[q], home(q, core, x), d_s.at[q], d_r.at[q], partner)

    def core_arrival(q):
        return remote(yrecv.at[q], home(q, 1 - core, x), d_s.at[q], d_r.at[q], partner)

    def relay(q):
        return remote(home(q, core, 1 - x), home(q, core, 1 - x), r_s.at[q], r_r.at[q], partner)

    def relay_arrival(q):
        return remote(home(q, 1 - core, 1 - x), home(q, 1 - core, 1 - x), r_s.at[q], r_r.at[q], partner)

    def local_copy(q):
        return pltpu.make_async_copy(yrecv.at[q], home(q, core, x), l_s.at[q])

    small = small_copies(phi_hbm, phi_ref, len_hbm, len_ref, small_sem)
    for copy in (*small, *load_w(0)):
        copy.start()
    for copy in small:
        copy.wait()
    v_ref[...] = unit_columns(phi_ref[...]).astype(BF16)
    greet((partner, across_x, across_y))
    for p in range(1, w_ring):
        for copy in load_w(p):
            copy.start()

    def expert_pair(p, carry):
        for copy in load_w(p):
            copy.wait()
        slot = lax.rem(p, w_ring)
        for j in range(2):
            e = 2 * p + j
            rows = gather_rows(xs_ref, pl.ds(pl.multiple_of(e * pitch, 8), n_batch)).astype(BF16)
            hidden = jnp.dot(rows, wi[slot, j], preferred_element_type=F32)
            hidden = (0.5 * hidden * (1.0 + lax.erf(hidden * math.sqrt(0.5)))).astype(BF16)
            out = jnp.dot(hidden, wo[slot, j], preferred_element_type=F32)
            g, first = e // group, pl.multiple_of(lax.rem(e, group) * (sub // 8), sub // 8)
            for bq in range(n_chunk):
                piece = out[bq * sub : (bq + 1) * sub].astype(BF16)
                ysend[lax.rem(g * n_chunk + bq, y_ring), pl.ds(first, sub // 8)] = piece.reshape(sub // 8, 8, dim)

        @pl.when(p < group // 2)
        def _():
            for bq in range(n_chunk):
                first_copy(p, bq).start()

        @pl.when(p + w_ring < n_pair)
        def _():
            for copy in load_w(p + w_ring):
                copy.start()

        return carry

    def mix_one(b):
        xv = xbuf[lax.rem(b, x_ring)]
        xf = xv.astype(F32)
        scale = lax.rsqrt(jnp.sum(xf * xf, axis=1, keepdims=True) + NORM_EPS) * kg
        logits = jnp.dot(xv, v_ref[...], preferred_element_type=F32) * scale
        weights = jnp.exp2(logits - jnp.max(logits, axis=1, keepdims=True))
        valid = lax.broadcasted_iota(jnp.int32, (tok, 1), 0) < len_ref[b] - s * tok
        inverse = jnp.where(valid, 1.0 / jnp.sum(weights, axis=1, keepdims=True), 0.0)
        c_ref[b] = (weights * inverse).astype(BF16)

    def mix_pair(m, carry):
        for j in range(2):
            load_x(2 * m + j).wait()
        for j in range(2):
            mix_one(2 * m + j)

        @pl.when(2 * m + x_ring < n_batch)
        def _():
            for j in range(2):
                load_x(2 * m + j + x_ring).start()

        return carry

    per = n_expert // n_q
    lag = 3
    n_mix = n_batch // 2
    early = 20

    def mix_start(t):
        first = jnp.maximum(t - n_chunk, 0) * early // (n_q - n_chunk)
        rest = early + (t - n_q) * (n_mix - early) // (lag + 3)
        return jnp.where(t < n_q, first, rest)

    def step(t, carry):
        @pl.when(t < n_q)
        def _():
            lax.fori_loop(t * (per // 2), (t + 1) * (per // 2), expert_pair, 0)

        @pl.when((t >= n_chunk) & (t < n_q) & (lax.rem(t, n_chunk) == n_chunk - 1))
        def _():
            for bq in range(n_chunk):
                y_copy(t - n_chunk + 1 + bq).start()

        @pl.when(t == 0)
        def _():
            for b in range(x_ring):
                load_x(b).start()

        lax.fori_loop(mix_start(t), mix_start(t + 1), mix_pair, 0)

        @pl.when((t >= lag) & (t < n_q + lag))
        def _():
            q = t - lag

            @pl.when(q < n_chunk)
            def _():
                for p in range(group // 2):
                    first_copy(p, q).wait_recv()

            @pl.when(q >= n_chunk)
            def _():
                y_copy(q).wait_recv()

            total = ysend[lax.rem(q, y_ring)].astype(F32) + yrecv[q].astype(F32)
            total = total.reshape(group * sub, dim)
            for e in range(group):
                scatter_rows(acc, e, group, total[e * sub : (e + 1) * sub])
            yrecv[q] = gather_rows(acc, pl.ds(0, group * sub)).reshape(sub, group, dim).astype(BF16)
            x_copy(q).start()
            core_copy(q).start()
            local_copy(q).start()

            @pl.when(q < n_chunk)
            def _():
                for p in range(group // 2):
                    first_copy(p, q).wait_send()

            @pl.when(q >= n_chunk)
            def _():
                y_copy(q).wait_send()

        @pl.when(t >= lag + 3)
        def _():
            q = t - lag - 3
            x_arrival(q).wait_recv()
            relay(q).start()

        return carry

    lax.fori_loop(0, n_q + lag + 3, step, 0)

    def drain(q, carry):
        core_arrival(q).wait_recv()
        relay_arrival(q).wait_recv()
        x_copy(q).wait_send()
        core_copy(q).wait_send()
        relay(q).wait_send()
        local_copy(q).wait()
        return carry

    lax.fori_loop(0, n_q, drain, 0)


def experts(tokens, phi, lengths, g, xs, w_in, w_out, pitch):
    n_batch, tok, dim = tokens.shape
    n_slots = phi.shape[1]
    n_expert, _, hid = w_in.shape
    n_group, n_chunk = 8, 2
    group, sub = n_expert // n_group, n_batch // n_chunk
    n_q = n_group * n_chunk
    x_ring, w_ring = 4, 3
    dma = pltpu.SemaphoreType.DMA
    vmem, smem, anym = pl.BlockSpec(memory_space=pltpu.VMEM), pl.BlockSpec(memory_space=pltpu.SMEM), pl.BlockSpec(memory_space=pl.ANY)
    return pl.pallas_call(
        functools.partial(expert_kernel, n_group, n_chunk, pitch),
        out_shape=(pltpu.VMEM((n_batch, tok, n_slots), BF16), jax.ShapeDtypeStruct((n_batch, n_slots, dim), BF16)),
        in_specs=[anym, anym, anym, smem, vmem, anym, anym],
        out_specs=(vmem, anym),
        scratch_shapes=[
            pltpu.VMEM((dim, n_slots), BF16),
            pltpu.SMEM((n_batch,), jnp.int32),
            pltpu.VMEM((dim, n_slots), BF16),
            pltpu.VMEM((x_ring, tok, dim), BF16),
            pltpu.VMEM((w_ring, 2, dim, hid), BF16),
            pltpu.VMEM((w_ring, 2, hid, dim), BF16),
            pltpu.VMEM((dim // 128, group * sub, 128), F32),
            pltpu.VMEM((n_q // 2, sub, group, dim), BF16),
            pltpu.VMEM((n_q, sub, group, dim), BF16),
            dma((2,)),
            dma((x_ring,)),
            dma((w_ring,)),
            dma((w_ring,)),
        ] + [dma((n_q,))] * 9 + [dma((group // 2 * n_chunk,))] * 2,
        compiler_params=pltpu.CompilerParams(collective_id=1, has_side_effects=True, vmem_limit_bytes=18 << 20),
        name="experts",
    )(tokens, phi, lengths, g, xs, w_in, w_out)


def combine_kernel(c_ref, ys_hbm, y_hbm, ys, out, ys_sem, y_sem):
    n_batch, ring = c_ref.shape[0], out.shape[0]
    depth, step = ys.shape[0], ys.shape[1]
    n_round = n_batch // ring

    def load(i, slot):
        return pltpu.make_async_copy(ys_hbm.at[pl.ds(i * step, step)], ys.at[slot], ys_sem.at[slot])

    def store(b, slot):
        return pltpu.make_async_copy(out.at[slot], y_hbm.at[b], y_sem.at[slot])

    for i in range(depth):
        load(i, i).start()

    def turn(r, carry):
        for i in range(depth):
            load(r * depth + i, i).wait()

            @pl.when(r > 0)
            def _():
                for j in range(i * step, (i + 1) * step):
                    store((r - 1) * ring + j, j).wait()

            for j in range(i * step, (i + 1) * step):
                out[j] = jnp.dot(c_ref[r * ring + j], ys[i, j - i * step], preferred_element_type=F32).astype(BF16)
            for j in range(i * step, (i + 1) * step):
                store(r * ring + j, j).start()

            @pl.when(r < n_round - 1)
            def _():
                load((r + 1) * depth + i, i).start()

        return carry

    lax.fori_loop(0, n_round, turn, 0)
    for j in range(ring):
        store(n_batch - ring + j, j).wait()


def combine(c, ys):
    n_batch, tok, n_slots = c.shape
    dim = ys.shape[2]
    step, depth, ring = 4, 4, 16
    return pl.pallas_call(
        combine_kernel,
        out_shape=jax.ShapeDtypeStruct((n_batch, tok, dim), BF16),
        in_specs=[pl.BlockSpec(memory_space=pltpu.VMEM), pl.BlockSpec(memory_space=pl.ANY)],
        out_specs=pl.BlockSpec(memory_space=pl.ANY),
        scratch_shapes=[
            pltpu.VMEM((depth, step, n_slots, dim), BF16),
            pltpu.VMEM((ring, tok, dim), BF16),
            pltpu.SemaphoreType.DMA((depth,)),
            pltpu.SemaphoreType.DMA((ring,)),
        ],
        compiler_params=pltpu.CompilerParams(vmem_limit_bytes=20 << 20),
        name="combine",
    )(c, ys)


def solution(mesh):
    def local_layer(tokens, lengths, slot_params, logit_scale, w_in, w_out):
        pitch = tokens.shape[0] + 8
        g = logit_scale.reshape(1)
        phi, lens = (pltpu.with_memory_space_constraint(a, pltpu.HBM) for a in (slot_params, lengths))
        xs = dispatch(tokens, phi, lens, g, pitch)
        c, ys = experts(tokens, phi, lens, g, pltpu.with_memory_space_constraint(xs, pltpu.VMEM), w_in, w_out, pitch)
        return combine(pltpu.with_memory_space_constraint(c, pltpu.VMEM), ys)

    return jax.shard_map(local_layer, mesh=mesh, in_specs=(P("data", "seq", None), P("data"), P(), P(), P("seq", None, "model"), P("seq", "model", None)), out_specs=P("data", "seq", None), check_vma=False)
```

```python
import functools
import math
import jax
import jax.numpy as jnp
from jax import lax
from jax.experimental import pallas as pl
from jax.experimental.pallas import tpu as pltpu
from jax.sharding import PartitionSpec as P

NORM_EPS = 1e-6
LOG2E = math.log2(math.e)
MASKED = -1e30
MESH = pl.DeviceIdType.MESH
F32, BF16 = jnp.float32, jnp.bfloat16
NT = (((1,), (1,)), ((), ()))


def unit_columns(values):
    v32 = values.astype(F32)
    return v32 * lax.rsqrt(jnp.sum(v32 * v32, axis=0, keepdims=True) + NORM_EPS)


def place():
    y, s = lax.axis_index("model"), lax.axis_index("seq")
    x, core = s // 2, lax.rem(s, 2)
    partner = (0, y, x * 2 + 1 - core)
    across_x = (0, y, (1 - x) * 2 + core)
    across_y = (0, 1 - y, s)
    return y, x, core, s, partner, across_x, across_y


def announce(devices):
    for device in devices:
        pl.semaphore_signal(pltpu.get_barrier_semaphore(), inc=1, device_id=device, device_id_type=MESH)


def greet(devices):
    announce(devices)
    pl.semaphore_wait(pltpu.get_barrier_semaphore(), len(devices))


def remote(src, dst, send, recv, device):
    return pltpu.make_async_remote_copy(src_ref=src, dst_ref=dst, send_sem=send, recv_sem=recv, device_id=device, device_id_type=MESH)


def small_copies(phi_hbm, phi_ref, len_hbm, len_ref, sem):
    return pltpu.make_async_copy(phi_hbm, phi_ref, sem.at[0]), pltpu.make_async_copy(len_hbm, len_ref, sem.at[1])


def merge_weights(a, b):
    top = jnp.maximum(a, b)
    ea, eb = jnp.exp2(a - top), jnp.exp2(b - top)
    total = ea + eb
    row = lax.broadcasted_iota(jnp.int32, (8, a.shape[1]), 0)
    weights = jnp.where(row == 0, ea, eb) * (1.0 / total)
    return jnp.transpose(weights), top + jnp.log2(total)


def scatter_rows(acc, first, stride, rows):
    for j in range(acc.shape[0]):
        acc[j, pl.ds(first, rows.shape[0], stride=stride), :] = rows[:, j * 128 : (j + 1) * 128]


def gather_rows(acc, rows):
    return jnp.concatenate([acc[j, rows, :] for j in range(acc.shape[0])], axis=1)


def dispatch_kernel(half, pitch, x_hbm, phi_hbm, len_hbm, g_ref, xs_ref, phi_ref, len_ref, vt_ref, xbuf, part, mid, xpart, own, yown, lse, dlse, mlse, xlse, wcol, small_sem, in_sem, d_s, d_r, dl_s, dl_r, x_s, x_r, xl_s, xl_r, y_s, y_r):
    size = part.shape[0] // d_s.shape[0]
    n_step = half // size
    tok, n_slots, dim = xbuf.shape[1], vt_ref.shape[0], xbuf.shape[2]
    core_slots, dev_slots = n_slots // 2, n_slots // 4
    y, x, core, s, partner, across_x, across_y = place()
    base = y * half
    ring = xbuf.shape[0]
    kg = g_ref[0] * LOG2E

    def load(i):
        slot = lax.rem(i, ring)
        return pltpu.make_async_copy(x_hbm.at[base + i], xbuf.at[slot], in_sem.at[slot])

    def core_copy(u):
        rows, some = pl.ds(pl.multiple_of((1 - core) * core_slots, core_slots), core_slots), pl.ds(u * size, size)
        return remote(part.at[some, rows], mid.at[some], d_s.at[u], d_r.at[u], partner)

    def core_lse(u):
        some = pl.ds(u * size, size)
        return remote(lse.at[1 - core, some], dlse.at[some], dl_s.at[u], dl_r.at[u], partner)

    def x_copy(u):
        rows, some = pl.ds(pl.multiple_of((1 - x) * dev_slots, dev_slots), dev_slots), pl.ds(u * size, size)
        return remote(mid.at[some, rows], xpart.at[some], x_s.at[u], x_r.at[u], across_x)

    def x_lse(u):
        some = pl.ds(u * size, size)
        return remote(mlse.at[some], xlse.at[some], xl_s.at[u], xl_r.at[u], across_x)

    def y_copy(u):
        some = pl.ds(u * size, size)
        return remote(own.at[some], yown.at[some], y_s.at[u], y_r.at[u], across_y)

    small = small_copies(phi_hbm, phi_ref, len_hbm, len_ref, small_sem)
    for copy in small:
        copy.start()
    for i in range(size):
        load(i).start()
    for copy in small:
        copy.wait()
    v_rows = jnp.transpose(unit_columns(phi_ref[...]))
    for j, block in enumerate((0, 2, 1, 3)):
        vt_ref[j * dev_slots : (j + 1) * dev_slots] = v_rows[block * dev_slots : (block + 1) * dev_slots].astype(BF16)
    greet((partner, across_x, across_y))
    for i in range(size, ring):
        load(i).start()

    def local_mean(i):
        xv = xbuf[lax.rem(i, ring)]
        xf = xv.astype(F32)
        square = jnp.sum(xf * xf, axis=1, keepdims=True)
        square_row = jnp.transpose(jnp.broadcast_to(square, (tok, 128)))[0:1]
        scale_row = lax.rsqrt(square_row + NORM_EPS) * kg
        logits = lax.dot_general(vt_ref[...], xv, NT, preferred_element_type=F32) * scale_row
        lane = lax.broadcasted_iota(jnp.int32, (1, tok), 1)
        masked = jnp.where(lane < len_ref[base + i] - s * tok, logits, MASKED)
        top = jnp.max(masked, axis=1, keepdims=True)
        weights = jnp.exp2(masked - top)
        total = jnp.sum(weights, axis=1, keepdims=True)
        mean = jnp.dot(weights.astype(BF16), xv, preferred_element_type=F32) * (1.0 / total)
        part[i] = mean.astype(BF16)
        first = lax.broadcasted_iota(jnp.int32, (n_slots, 128), 1) == 0
        rows = jnp.transpose(jnp.where(first, top, total))
        row = rows[0:1] + jnp.log2(rows[1:2])
        lse[0, i] = row[:, :core_slots]
        lse[1, i] = row[:, core_slots:]

    def step(u, carry):
        @pl.when(u < n_step)
        def _():
            for j in range(size):
                load(u * size + j).wait()
            for j in range(size):
                local_mean(u * size + j)
            core_copy(u).start()
            core_lse(u).start()

            @pl.when(u * size + ring < half)
            def _():
                for j in range(size):
                    load(u * size + j + ring).start()

        def core_wait():
            core_copy(u - 1).wait_recv()
            core_lse(u - 1).wait_recv()

        def core_merge():
            rows = pl.ds(pl.multiple_of(core * core_slots, core_slots), core_slots)
            for j in range(size):
                k = (u - 1) * size + j
                cols, row = merge_weights(lse[core, k], dlse[k])
                merged = cols[:, 0:1] * part[k, rows].astype(F32) + cols[:, 1:2] * mid[k].astype(F32)
                mid[k] = merged.astype(BF16)
                mlse[k] = row

        def core_send():
            x_copy(u - 1).start()
            x_lse(u - 1).start()

        def x_wait():
            x_copy(u - 3).wait_recv()
            x_lse(u - 3).wait_recv()

        def x_merge():
            rows = pl.ds(pl.multiple_of(x * dev_slots, dev_slots), dev_slots)
            for j in range(size):
                k = (u - 3) * size + j
                cols, _ = merge_weights(mlse[k], xlse[k])
                wcol[j] = cols
                mine = wcol[j, rows, :]
                merged = mine[:, 0:1] * mid[k, rows].astype(F32) + mine[:, 1:2] * xpart[k].astype(F32)
                own[k] = merged.astype(BF16)
                scatter_rows(xs_ref, base + k, pitch, merged)

        def y_place():
            for j in range(size):
                k = (u - 5) * size + j
                scatter_rows(xs_ref, (1 - y) * half + k, pitch, yown[k].astype(F32))

        steady = (u >= 5) & (u <= n_step)

        @pl.when(steady)
        def _():
            core_wait()
            x_wait()
            y_copy(u - 5).wait_recv()
            core_merge()
            x_merge()
            y_place()
            core_send()
            y_copy(u - 3).start()

        @pl.when((u >= 1) & (u < 5))
        def _():
            core_wait()
            core_merge()
            core_send()

        @pl.when((u >= 3) & (u < n_step + 3) & jnp.logical_not(steady))
        def _():
            x_wait()
            x_merge()
            y_copy(u - 3).start()

        @pl.when(u > n_step)
        def _():
            y_copy(u - 5).wait_recv()
            y_place()

        return carry

    lax.fori_loop(0, n_step + 5, step, 0)

    def drain(u, carry):
        core_copy(u).wait_send()
        core_lse(u).wait_send()
        x_copy(u).wait_send()
        x_lse(u).wait_send()
        y_copy(u).wait_send()
        return carry

    lax.fori_loop(0, n_step, drain, 0)


def dispatch(tokens, phi, lengths, g, pitch):
    n_batch, tok, dim = tokens.shape
    n_slots = phi.shape[1]
    half, ring, size = n_batch // 2, 4, 2
    dma = pltpu.SemaphoreType.DMA
    return pl.pallas_call(
        functools.partial(dispatch_kernel, half, pitch),
        out_shape=pltpu.VMEM((dim // 128, n_slots // 4 * pitch, 128), F32),
        in_specs=[pl.BlockSpec(memory_space=pl.ANY)] * 3 + [pl.BlockSpec(memory_space=pltpu.SMEM)],
        out_specs=pl.BlockSpec(memory_space=pltpu.VMEM),
        scratch_shapes=[
            pltpu.VMEM((dim, n_slots), BF16),
            pltpu.SMEM((n_batch,), jnp.int32),
            pltpu.VMEM((n_slots, dim), BF16),
            pltpu.VMEM((ring, tok, dim), BF16),
            pltpu.VMEM((half, n_slots, dim), BF16),
            pltpu.VMEM((half, n_slots // 2, dim), BF16),
            pltpu.VMEM((half, n_slots // 4, dim), BF16),
            pltpu.VMEM((half, n_slots // 4, dim), BF16),
            pltpu.VMEM((half, n_slots // 4, dim), BF16),
            pltpu.VMEM((2, half, 1, n_slots // 2), F32),
            pltpu.VMEM((half, 1, n_slots // 2), F32),
            pltpu.VMEM((half, 1, n_slots // 2), F32),
            pltpu.VMEM((half, 1, n_slots // 2), F32),
            pltpu.VMEM((size, n_slots // 2, 8), F32),
            dma((2,)),
            dma((ring,)),
        ] + [dma((half // size,))] * 10,
        compiler_params=pltpu.CompilerParams(collective_id=0, has_side_effects=True, vmem_limit_bytes=20 << 20),
        name="dispatch",
    )(tokens, phi, lengths, g)


def expert_kernel(n_group, n_chunk, pitch, x_hbm, phi_hbm, len_hbm, g_ref, xs_ref, win_hbm, wout_hbm, c_ref, ys_hbm, phi_ref, len_ref, v_ref, xbuf, wi, wo, acc, ysend, yrecv, small_sem, x_sem, wi_sem, wo_sem, y_s, y_r, x_s, x_r, d_s, d_r, r_s, r_r, l_s, f_s, f_r):
    n_batch, tok, dim = x_hbm.shape
    n_expert = win_hbm.shape[0]
    group = n_expert // n_group
    sub = n_batch // n_chunk
    kg = g_ref[0] * LOG2E
    y, x, core, s, partner, across_x, across_y = place()
    x_ring, w_ring, y_ring = xbuf.shape[0], wi.shape[0], ysend.shape[0]
    n_pair = n_expert // 2
    n_q = n_group * n_chunk

    def load_x(b):
        slot = lax.rem(b, x_ring)
        return pltpu.make_async_copy(x_hbm.at[b], xbuf.at[slot], x_sem.at[slot])

    def load_w(p):
        slot = lax.rem(p, w_ring)
        return (
            pltpu.make_async_copy(win_hbm.at[pl.ds(2 * p, 2)], wi.at[slot], wi_sem.at[slot]),
            pltpu.make_async_copy(wout_hbm.at[pl.ds(2 * p, 2)], wo.at[slot], wo_sem.at[slot]),
        )

    def home(q, on_core, on_x):
        g, bq = q // n_chunk, lax.rem(q, n_chunk)
        slot0 = pl.multiple_of((on_x * 2 + on_core) * n_expert + g * group, group)
        return ys_hbm.at[pl.ds(bq * sub, sub), pl.ds(slot0, group)]

    def y_copy(q):
        return remote(ysend.at[lax.rem(q, y_ring)], yrecv.at[q], y_s.at[q], y_r.at[q], across_y)

    def first_copy(p, bq):
        some, k = pl.ds(p * (sub // 4), sub // 4), p * n_chunk + bq
        return remote(ysend.at[bq, some], yrecv.at[bq, some], f_s.at[k], f_r.at[k], across_y)

    def x_copy(q):
        return remote(yrecv.at[q], home(q, core, x), x_s.at[q], x_r.at[q], across_x)

    def x_arrival(q):
        return remote(yrecv.at[q], home(q, core, 1 - x), x_s.at[q], x_r.at[q], across_x)

    def core_copy(q):
        return remote(yrecv.at[q], home(q, core, x), d_s.at[q], d_r.at[q], partner)

    def core_arrival(q):
        return remote(yrecv.at[q], home(q, 1 - core, x), d_s.at[q], d_r.at[q], partner)

    def relay(q):
        return remote(home(q, core, 1 - x), home(q, core, 1 - x), r_s.at[q], r_r.at[q], partner)

    def relay_arrival(q):
        return remote(home(q, 1 - core, 1 - x), home(q, 1 - core, 1 - x), r_s.at[q], r_r.at[q], partner)

    def local_copy(q):
        return pltpu.make_async_copy(yrecv.at[q], home(q, core, x), l_s.at[q])

    small = small_copies(phi_hbm, phi_ref, len_hbm, len_ref, small_sem)
    for copy in (*small, *load_w(0)):
        copy.start()
    for copy in small:
        copy.wait()
    v_ref[...] = unit_columns(phi_ref[...]).astype(BF16)
    announce((partner, across_x, across_y))
    for p in range(1, w_ring):
        for copy in load_w(p):
            copy.start()

    def expert_pair(p, carry):
        for copy in load_w(p):
            copy.wait()
        slot = lax.rem(p, w_ring)
        for j in range(2):
            e = 2 * p + j
            rows = gather_rows(xs_ref, pl.ds(pl.multiple_of(e * pitch, 8), n_batch)).astype(BF16)
            hidden = jnp.dot(rows, wi[slot, j], preferred_element_type=F32)
            hidden = (0.5 * hidden * (1.0 + lax.erf(hidden * math.sqrt(0.5)))).astype(BF16)
            out = jnp.dot(hidden, wo[slot, j], preferred_element_type=F32)
            g, first = e // group, pl.multiple_of(lax.rem(e, group) * (sub // 8), sub // 8)
            for bq in range(n_chunk):
                piece = out[bq * sub : (bq + 1) * sub].astype(BF16)
                ysend[lax.rem(g * n_chunk + bq, y_ring), pl.ds(first, sub // 8)] = piece.reshape(sub // 8, 8, dim)

        @pl.when(p == 0)
        def _():
            pl.semaphore_wait(pltpu.get_barrier_semaphore(), 3)

        @pl.when(p < group // 2)
        def _():
            for bq in range(n_chunk):
                first_copy(p, bq).start()

        @pl.when(p + w_ring < n_pair)
        def _():
            for copy in load_w(p + w_ring):
                copy.start()

        return carry

    def mix_one(b):
        xv = xbuf[lax.rem(b, x_ring)]
        xf = xv.astype(F32)
        scale = lax.rsqrt(jnp.sum(xf * xf, axis=1, keepdims=True) + NORM_EPS) * kg
        logits = jnp.dot(xv, v_ref[...], preferred_element_type=F32) * scale
        weights = jnp.exp2(logits - jnp.max(logits, axis=1, keepdims=True))
        valid = lax.broadcasted_iota(jnp.int32, (tok, 1), 0) < len_ref[b] - s * tok
        inverse = jnp.where(valid, 1.0 / jnp.sum(weights, axis=1, keepdims=True), 0.0)
        c_ref[b] = (weights * inverse).astype(BF16)

    def mix_pair(m, carry):
        for j in range(2):
            load_x(2 * m + j).wait()
        for j in range(2):
            mix_one(2 * m + j)

        @pl.when(2 * m + x_ring < n_batch)
        def _():
            for j in range(2):
                load_x(2 * m + j + x_ring).start()

        return carry

    per = n_expert // n_q
    lag = 3
    n_mix = n_batch // 2
    early = 20

    def mix_start(t):
        first = jnp.maximum(t - n_chunk, 0) * early // (n_q - n_chunk)
        rest = early + (t - n_q) * (n_mix - early) // (lag + 3)
        return jnp.where(t < n_q, first, rest)

    def step(t, carry):
        @pl.when(t < n_q)
        def _():
            lax.fori_loop(t * (per // 2), (t + 1) * (per // 2), expert_pair, 0)

        @pl.when((t >= n_chunk) & (t < n_q) & (lax.rem(t, n_chunk) == n_chunk - 1))
        def _():
            for bq in range(n_chunk):
                y_copy(t - n_chunk + 1 + bq).start()

        @pl.when(t == 0)
        def _():
            for b in range(x_ring):
                load_x(b).start()

        lax.fori_loop(mix_start(t), mix_start(t + 1), mix_pair, 0)

        @pl.when((t >= lag) & (t < n_q + lag))
        def _():
            q = t - lag

            @pl.when(q < n_chunk)
            def _():
                for p in range(group // 2):
                    first_copy(p, q).wait_recv()

            @pl.when(q >= n_chunk)
            def _():
                y_copy(q).wait_recv()

            total = ysend[lax.rem(q, y_ring)].astype(F32) + yrecv[q].astype(F32)
            total = total.reshape(group * sub, dim)
            for e in range(group):
                scatter_rows(acc, e, group, total[e * sub : (e + 1) * sub])
            yrecv[q] = gather_rows(acc, pl.ds(0, group * sub)).reshape(sub, group, dim).astype(BF16)
            x_copy(q).start()
            core_copy(q).start()
            local_copy(q).start()

            @pl.when(q < n_chunk)
            def _():
                for p in range(group // 2):
                    first_copy(p, q).wait_send()

            @pl.when(q >= n_chunk)
            def _():
                y_copy(q).wait_send()

        @pl.when(t >= lag + 3)
        def _():
            q = t - lag - 3
            x_arrival(q).wait_recv()
            relay(q).start()

        return carry

    lax.fori_loop(0, n_q + lag + 3, step, 0)

    def drain(q, carry):
        core_arrival(q).wait_recv()
        relay_arrival(q).wait_recv()
        x_copy(q).wait_send()
        core_copy(q).wait_send()
        relay(q).wait_send()
        local_copy(q).wait()
        return carry

    lax.fori_loop(0, n_q, drain, 0)


def experts(tokens, phi, lengths, g, xs, w_in, w_out, pitch):
    n_batch, tok, dim = tokens.shape
    n_slots = phi.shape[1]
    n_expert, _, hid = w_in.shape
    n_group, n_chunk = 8, 2
    group, sub = n_expert // n_group, n_batch // n_chunk
    n_q = n_group * n_chunk
    x_ring, w_ring = 4, 3
    dma = pltpu.SemaphoreType.DMA
    vmem, smem, anym = pl.BlockSpec(memory_space=pltpu.VMEM), pl.BlockSpec(memory_space=pltpu.SMEM), pl.BlockSpec(memory_space=pl.ANY)
    return pl.pallas_call(
        functools.partial(expert_kernel, n_group, n_chunk, pitch),
        out_shape=(pltpu.VMEM((n_batch, tok, n_slots), BF16), jax.ShapeDtypeStruct((n_batch, n_slots, dim), BF16)),
        in_specs=[anym, anym, anym, smem, vmem, anym, anym],
        out_specs=(vmem, anym),
        scratch_shapes=[
            pltpu.VMEM((dim, n_slots), BF16),
            pltpu.SMEM((n_batch,), jnp.int32),
            pltpu.VMEM((dim, n_slots), BF16),
            pltpu.VMEM((x_ring, tok, dim), BF16),
            pltpu.VMEM((w_ring, 2, dim, hid), BF16),
            pltpu.VMEM((w_ring, 2, hid, dim), BF16),
            pltpu.VMEM((dim // 128, group * sub, 128), F32),
            pltpu.VMEM((n_q // 2, sub, group, dim), BF16),
            pltpu.VMEM((n_q, sub, group, dim), BF16),
            dma((2,)),
            dma((x_ring,)),
            dma((w_ring,)),
            dma((w_ring,)),
        ] + [dma((n_q,))] * 9 + [dma((group // 2 * n_chunk,))] * 2,
        compiler_params=pltpu.CompilerParams(collective_id=1, has_side_effects=True, vmem_limit_bytes=18 << 20),
        name="experts",
    )(tokens, phi, lengths, g, xs, w_in, w_out)


def combine_kernel(c_ref, ys_hbm, y_hbm, ys, out, ys_sem, y_sem):
    n_batch, ring = c_ref.shape[0], out.shape[0]
    depth, step = ys.shape[0], ys.shape[1]
    n_round = n_batch // ring

    def load(i, slot):
        return pltpu.make_async_copy(ys_hbm.at[pl.ds(i * step, step)], ys.at[slot], ys_sem.at[slot])

    def store(b, slot):
        return pltpu.make_async_copy(out.at[slot], y_hbm.at[b], y_sem.at[slot])

    for i in range(depth):
        load(i, i).start()

    def turn(r, carry):
        for i in range(depth):
            load(r * depth + i, i).wait()

            @pl.when(r > 0)
            def _():
                for j in range(i * step, (i + 1) * step):
                    store((r - 1) * ring + j, j).wait()

            for j in range(i * step, (i + 1) * step):
                out[j] = jnp.dot(c_ref[r * ring + j], ys[i, j - i * step], preferred_element_type=F32).astype(BF16)
            for j in range(i * step, (i + 1) * step):
                store(r * ring + j, j).start()

            @pl.when(r < n_round - 1)
            def _():
                load((r + 1) * depth + i, i).start()

        return carry

    lax.fori_loop(0, n_round, turn, 0)
    for j in range(ring):
        store(n_batch - ring + j, j).wait()


def combine(c, ys):
    n_batch, tok, n_slots = c.shape
    dim = ys.shape[2]
    step, depth, ring = 4, 4, 16
    return pl.pallas_call(
        combine_kernel,
        out_shape=jax.ShapeDtypeStruct((n_batch, tok, dim), BF16),
        in_specs=[pl.BlockSpec(memory_space=pltpu.VMEM), pl.BlockSpec(memory_space=pl.ANY)],
        out_specs=pl.BlockSpec(memory_space=pl.ANY),
        scratch_shapes=[
            pltpu.VMEM((depth, step, n_slots, dim), BF16),
            pltpu.VMEM((ring, tok, dim), BF16),
            pltpu.SemaphoreType.DMA((depth,)),
            pltpu.SemaphoreType.DMA((ring,)),
        ],
        compiler_params=pltpu.CompilerParams(vmem_limit_bytes=20 << 20),
        name="combine",
    )(c, ys)


def solution(mesh):
    def local_layer(tokens, lengths, slot_params, logit_scale, w_in, w_out):
        pitch = tokens.shape[0] + 8
        g = logit_scale.reshape(1)
        phi, lens = (pltpu.with_memory_space_constraint(a, pltpu.HBM) for a in (slot_params, lengths))
        xs = dispatch(tokens, phi, lens, g, pitch)
        c, ys = experts(tokens, phi, lens, g, pltpu.with_memory_space_constraint(xs, pltpu.VMEM), w_in, w_out, pitch)
        return combine(pltpu.with_memory_space_constraint(c, pltpu.VMEM), ys)

    return jax.shard_map(local_layer, mesh=mesh, in_specs=(P("data", "seq", None), P("data"), P(), P(), P("seq", None, "model"), P("seq", "model", None)), out_specs=P("data", "seq", None), check_vma=False)
```
